32 devices in a mesh: angle: 2 (over y), row: 8 (over z, x), col: 2 (over core).
Axes of the slice: x: 2, y: 2, z: 4, core: 2. Of those that a mesh axis runs over, the one named last changes fastest.
Arguments:
- obj_field: float32 [2, 2048, 1024], P(None, ('angle', 'row'), 'col'), parts along dimension 1, may hold values from -6 to 6
- probe_modes: bfloat16 [2, 6, 256, 256], replicated, may hold values from -6 to 6
- centers: int32 [32, 2], P(('angle', 'row', 'col')), parts along dimension 0, may hold values from 0 to 1023, as said below
- amplitudes: float32 [32, 256, 256], P(('angle', 'row', 'col')), parts along dimension 0, may hold values from 0.2 to 4
Outputs:
- new_object: float32 [2, 2048, 1024], P(None, ('angle', 'row'), 'col'), parts along dimension 1
- new_probe: float32 [2, 12, 256, 256], P(None, 'angle'), parts along dimension 1
The draws below stay inside these ranges and needn't reach their ends.
There are 2 independent parts, one for each index of `angle`. The reference program is written for one: setup_inputs(seed, part) draws one part's arguments, and reference() takes and returns one part's arrays. A program takes and returns all parts, laid end to end along the dimension named above; an argument that names none is the same for every part. Nothing has to cross between parts.
Inputs may be any that keep to these rules, and one draw needn't show every extreme that they name: `centers`: position k belongs to device d = k // 1 of the row+col order (row slowest); its centre lies in that device's tile: row in [(d // (1024 // 512)) * 128, + 128), column in [(d % (1024 // 512)) * 512, + 512).
All inputs are finite; a program needn't handle non-finite values.
Results may differ from the reference program's by a relative error of at most 0.0003.
Values sent between devices are 32-bit elements; how exact they have to be, the bound alone decides.
A program may use at most 64 MiB of HBM per device.

```python
import math
import jax
import jax.numpy as jnp
from jax import lax

P_SIZE = 256
MODES = 6
TILE_R = 128
TILE_C = 512
POS_DEV = 1
OBJ_ROWS = 1024
OBJ_COLS = 1024
POSITIONS = 16


def draw_centers(key, part):
    first_key, second_key = jax.random.split(jax.random.fold_in(key, 11))
    owner = jnp.arange(POSITIONS, dtype=jnp.int32) // POS_DEV
    tiles_across = OBJ_COLS // TILE_C
    tile_row = owner // tiles_across
    tile_col = owner % tiles_across
    rows_drawn = tile_row * TILE_R + jax.random.randint(first_key, (POSITIONS,), 0, TILE_R)
    cols_drawn = tile_col * TILE_C + jax.random.randint(second_key, (POSITIONS,), 0, TILE_C)
    return jnp.stack([rows_drawn, cols_drawn], axis=1).astype(jnp.int32)


def steps_of(key, extent, cuts, smallest, largest):
    def one(axis_at, shards_of):
        steps = jax.random.uniform(jax.random.fold_in(jax.random.fold_in(key, 6), axis_at), (shards_of,), jnp.float32, smallest / len(cuts), largest / len(cuts))
        return jnp.repeat(jnp.exp(steps), extent[axis_at] // shards_of).reshape((-1,) + (1,) * (len(extent) - axis_at - 1))

    gain = one(*cuts[0])
    for cut in cuts[1:]:
        gain = gain * one(*cut)
    return gain


def scatter_about(own_key, extent, width, most, shards=(), kind=jnp.bfloat16):
    gain = steps_of(own_key, extent, shards, -0.22, 0.18) if shards else 1.0
    entries = jax.random.normal(own_key, extent, jnp.float32) * width * gain
    return jnp.minimum(jnp.maximum(entries, -most), most).astype(kind)


def setup_inputs(seed: int = 0, part: int = 0) -> dict:
    splits = jax.random.split(jax.random.key(seed), 5)
    own_keys = jax.random.split(jax.random.fold_in(splits[4], part), 5)
    return {
        "obj_field": scatter_about(own_keys[0], (2, OBJ_ROWS, OBJ_COLS), 1.0, 6.0, ((1, 8), (2, 2)), jnp.float32),
        "probe_modes": scatter_about(splits[1], (2, MODES, P_SIZE, P_SIZE), 1.0, 6.0),
        "centers": draw_centers(jax.random.fold_in(jax.random.fold_in(splits[4], part), 71), part),
        "amplitudes": jnp.clip(jnp.exp(math.log(4.0) - 2.9957323 * jax.random.uniform(own_keys[3], (POSITIONS, P_SIZE, P_SIZE), jnp.float32) ** steps_of(own_keys[3], (POSITIONS, P_SIZE, P_SIZE), ((0, 16),), -0.2, 0.2)), 0.2, 4.0),
    }


def reference(obj_field, probe_modes, centers, amplitudes):
    margin = P_SIZE // 2
    probe = probe_modes.astype(jnp.float32)
    probe_real = probe[0]
    probe_imag = probe[1]
    spot_map = lax.optimization_barrier(jnp.sum(probe_real * probe_real + probe_imag * probe_imag, axis=0))
    padded = jnp.pad(obj_field, ((0, 0), (margin, margin), (margin, margin)))
    anchor = jnp.zeros((), jnp.int32)

    def visit_position(totals, inputs):
        buffer, probe_grad, probe_weight = totals
        center, measured = inputs
        row_start = center[0].astype(jnp.int32)
        col_start = center[1].astype(jnp.int32)
        window = lax.dynamic_slice(padded, (anchor, row_start, col_start), (2, P_SIZE, P_SIZE))
        win_real = window[0]
        win_imag = window[1]
        exit_real = probe_real * win_real - probe_imag * win_imag
        exit_imag = probe_real * win_imag + probe_imag * win_real
        far_field = jnp.fft.fft2(lax.complex(exit_real, exit_imag), norm='ortho')
        far_real = jnp.real(far_field)
        far_imag = jnp.imag(far_field)
        modulus = jnp.sqrt(lax.optimization_barrier(jnp.sum(far_real * far_real + far_imag * far_imag, axis=0)))
        factor = measured / (modulus + 0.5)
        back_wave = jnp.fft.ifft2(lax.complex(far_real * factor, far_imag * factor), norm='ortho')
        diff_real = jnp.real(back_wave) - exit_real
        diff_imag = jnp.imag(back_wave) - exit_imag
        obj_real = lax.optimization_barrier(jnp.sum(probe_real * diff_real + probe_imag * diff_imag, axis=0))
        obj_imag = lax.optimization_barrier(jnp.sum(probe_real * diff_imag - probe_imag * diff_real, axis=0))
        stacked = jnp.stack([obj_real, obj_imag, spot_map])
        current = lax.dynamic_slice(buffer, (anchor, row_start, col_start), (3, P_SIZE, P_SIZE))
        buffer = lax.dynamic_update_slice(buffer, current + stacked, (anchor, row_start, col_start))
        probe_grad = probe_grad + jnp.stack([win_real * diff_real + win_imag * diff_imag, win_real * diff_imag - win_imag * diff_real])
        probe_weight = probe_weight + win_real * win_real + win_imag * win_imag
        return ((buffer, probe_grad, probe_weight), None)
    start_state = (jnp.zeros((3, OBJ_ROWS + 2 * margin, OBJ_COLS + 2 * margin), jnp.float32), jnp.zeros((2, MODES, P_SIZE, P_SIZE), jnp.float32), jnp.zeros((P_SIZE, P_SIZE), jnp.float32))
    final_state, unused = lax.scan(visit_position, start_state, (centers, amplitudes))
    buffer, probe_grad, probe_weight = final_state
    interior = buffer[:, margin:margin + OBJ_ROWS, margin:margin + OBJ_COLS]
    illumination = interior[2]
    peak_value = jnp.max(illumination)
    new_object = obj_field + interior[:2] / (illumination + 0.1 * peak_value)
    peak_weight = jnp.max(probe_weight)
    new_probe = probe + probe_grad / (probe_weight + 0.1 * peak_weight)
    return (new_object, new_probe)
```

```python
import functools
import math

import jax
import jax.numpy as jnp
import numpy as np
from jax import lax
from jax.experimental import pallas as pl
from jax.experimental.pallas import tpu as pltpu
from jax.sharding import PartitionSpec as P

MESH = pl.DeviceIdType.MESH
F32 = jnp.float32
BF16 = jnp.bfloat16
VMEM = pl.BlockSpec(memory_space=pltpu.VMEM)
SMEM = pl.BlockSpec(memory_space=pltpu.SMEM)
LIMIT = 60 * 1024 * 1024


def padded(block, sides, width):
    for axis, dim in sides:
        count = lax.axis_size(axis)
        forward = [(i, i + 1) for i in range(count - 1)]
        backward = [(target, source) for source, target in forward]
        low = lax.ppermute(
            lax.slice_in_dim(block, block.shape[dim] - width, None, axis=dim), axis, forward
        )
        high = lax.ppermute(lax.slice_in_dim(block, 0, width, axis=dim), axis, backward)
        block = jnp.concatenate([low, block, high], axis=dim)
    return block


def split(x):
    high = x.astype(BF16)
    return high, (x - high.astype(F32)).astype(BF16)


def dot(a, b):
    return jnp.dot(a, b, preferred_element_type=F32)


def dot3(a, b):
    return dot(a[0], b[1]) + dot(a[1], b[0]) + dot(a[0], b[0])


def tables(side):
    half = side // 2
    k = np.arange(half)
    phase = (k[:, None] * k[None, :] % half) * (2.0 * math.pi / half)
    scale = 1.0 / math.sqrt(side)
    cosine, sine = np.cos(phase) * scale, np.sin(phase) * scale
    matrix = np.block([[cosine, sine], [-sine, cosine]]).astype(np.float32)
    turn = k * (2.0 * math.pi / side)
    lanes = np.stack([np.cos(turn), np.sin(turn)]).astype(np.float32)
    rows = np.broadcast_to(lanes[:, :, None], (2, half, side))
    order = np.concatenate([np.arange(0, side, 2), np.arange(1, side, 2)])
    shuffle = (np.arange(side)[:, None] == order[None, :]).astype(np.float32)
    high = matrix.astype(BF16)
    low = (matrix - high.astype(np.float32)).astype(BF16)
    return (
        jnp.asarray(np.stack([high, low])),
        jnp.asarray(np.stack([high.T, low.T])),
        jnp.asarray(rows),
        jnp.asarray(lanes),
        jnp.asarray(np.stack([shuffle, shuffle.T])).astype(BF16),
    )


def cat(parts, axis):
    return jnp.concatenate(parts, axis=axis)


def forward_transform(re, im, a, b, rows, lanes):
    h = re.shape[0] // 2
    n = 2 * h
    er, ei = re[:h] + re[h:], im[:h] + im[h:]
    dr, di = re[:h] - re[h:], im[:h] - im[h:]
    c, s = rows
    stacked = cat([cat([er, dr * c + di * s], 1), cat([ei, di * c - dr * s], 1)], 0)
    y = dot3(a, split(stacked))
    yr = cat([y[:h, :n], y[:h, n:]], 0)
    yi = cat([y[h:, :n], y[h:, n:]], 0)
    er, ei = yr[:, :h] + yr[:, h:], yi[:, :h] + yi[:, h:]
    dr, di = yr[:, :h] - yr[:, h:], yi[:, :h] - yi[:, h:]
    c, s = lanes
    stacked = cat([cat([er, ei], 1), cat([dr * c + di * s, di * c - dr * s], 1)], 0)
    z = dot3(split(stacked), b)
    return cat([z[:n, :h], z[n:, :h]], 1), cat([z[:n, h:], z[n:, h:]], 1)


def inverse_transform(fr, fi, a, b, rows, lanes):
    h = fr.shape[0] // 2
    n = 2 * h
    stacked = cat([cat([fr[:, :h], fi[:, :h]], 1), cat([fr[:, h:], fi[:, h:]], 1)], 0)
    z = dot3(split(stacked), a)
    er, ei, odr, odi = z[:n, :h], z[:n, h:], z[n:, :h], z[n:, h:]
    c, s = lanes
    tr, ti = odr * c - odi * s, odi * c + odr * s
    yr = cat([er + tr, er - tr], 1)
    yi = cat([ei + ti, ei - ti], 1)
    stacked = cat([cat([yr[:h], yr[h:]], 1), cat([yi[:h], yi[h:]], 1)], 0)
    v = dot3(b, split(stacked))
    er, ei, odr, odi = v[:h, :n], v[h:, :n], v[:h, n:], v[h:, n:]
    c, s = rows
    tr, ti = odr * c - odi * s, odi * c + odr * s
    return cat([er + tr, er - tr], 0), cat([ei + ti, ei - ti], 0)


def row_picker(count, depth, start, valid):
    place = lax.broadcasted_iota(jnp.int32, (count, depth), 0) - lax.broadcasted_iota(
        jnp.int32, (count, depth), 1
    )
    hit = (place == start) & (valid != 0)
    return jnp.where(hit, 1.0, 0.0).astype(BF16)


def col_picker(depth, count, start):
    place = lax.broadcasted_iota(jnp.int32, (depth, count), 1) - lax.broadcasted_iota(
        jnp.int32, (depth, count), 0
    )
    return jnp.where(place == start, 1.0, 0.0).astype(BF16)


def update_kernel(
    places, window, probe, amp, a_ref, b_ref, rows_ref, lanes_ref, shuffle,
    grad, numer, illum, peak, far, power,
):
    modes, side = probe.shape[1], probe.shape[2]
    half = side // 2
    a = (a_ref[0], a_ref[1])
    b = (b_ref[0], b_ref[1])
    rows = (rows_ref[0], rows_ref[1])
    lanes = (lanes_ref[0:1, :], lanes_ref[1:2, :])

    def wave(m):
        pr, pi = probe[0, m].astype(F32), probe[1, m].astype(F32)
        wr, wi = window[0], window[1]
        return pr, pi, wr, wi, pr * wr - pi * wi, pr * wi + pi * wr

    power[...] = jnp.zeros_like(power)

    def ahead(m, carry):
        pr, pi, wr, wi, xr, xi = wave(m)
        fr, fi = forward_transform(xr, xi, a, b, rows, lanes)
        far[0, m] = fr
        far[1, m] = fi
        power[0] += fr * fr + fi * fi
        power[1] += pr * pr + pi * pi
        return carry

    lax.fori_loop(0, modes, ahead, 0)
    measured = 0.0
    rest = amp[...]
    for i in range(3):
        piece = rest.astype(BF16)
        rest = rest - piece.astype(F32)
        measured += dot(dot(shuffle[1], piece).astype(BF16), shuffle[0])
    power[0] = measured / (jnp.sqrt(power[0]) + 0.5)
    high, low = split(power[1])
    tile_rows, tile_cols = illum.shape
    spot = cat([high, low], 1)
    illum[...] = jnp.zeros_like(illum)

    def place_spot(k, carry):
        picked = dot(row_picker(tile_rows, side, places[k, 0], places[k, 2]), spot).astype(BF16)
        across = col_picker(side, tile_cols, places[k, 1])
        placed = dot(cat([picked[:, :side], picked[:, side:]], 0), across)
        illum[...] += placed[:tile_rows] + placed[tile_rows:]
        return carry

    lax.fori_loop(0, places.shape[0], place_spot, 0)
    peak[...] = jnp.full(peak.shape, jnp.max(illum[...]), F32)
    numer[...] = jnp.zeros_like(numer)

    def back(m, carry):
        pr, pi, wr, wi, xr, xi = wave(m)
        factor = power[0]
        gr, gi = inverse_transform(far[0, m] * factor, far[1, m] * factor, a, b, rows, lanes)
        dr, di = gr - xr, gi - xi
        numer[0] += pr * dr + pi * di
        numer[1] += pr * di - pi * dr
        ur = wr * dr + wi * di
        ui = wr * di - wi * dr
        for t in range(2):
            grad[t, pl.ds(pl.multiple_of(m * half, half), half), :] = ur[t * half : (t + 1) * half]
            grad[t, pl.ds(pl.multiple_of((modes + m) * half, half), half), :] = ui[
                t * half : (t + 1) * half
            ]
        return carry

    lax.fori_loop(0, modes, back, 0)
    weight = window[0] * window[0] + window[1] * window[1]
    top = 2 * modes * half
    for t in range(2):
        grad[t, top : top + half, :] = weight[t * half : (t + 1) * half]
        if grad.shape[1] > top + half:
            grad[t, top + half :, :] = jnp.zeros((grad.shape[1] - top - half, side), F32)


def ring_split(lines, ring):
    chunk = -(-lines // (16 * ring)) * 8
    pieces = min(4, chunk // 8)
    offsets, at = [], 0
    for i in range(pieces):
        size = (chunk // 8 // pieces + (1 if i < chunk // 8 % pieces else 0)) * 8
        offsets.append((at, size))
        at += size
    return chunk, offsets


def exchange_kernel(
    ring, chunk, pieces, grad, numer, peak, total, rims, mate, top,
    own, inbox, other, peaks, core_s, core_r, rs_s, rs_r, ag_s, ag_r, dd_s, dd_r,
    rim_s, rim_r, fwd_s, fwd_r, pk_s, pk_r,
):
    row, col = lax.axis_index("row"), lax.axis_index("col")
    side = grad.shape[2]
    half = side // 2
    mine = col
    odd = lax.rem(row, 2)
    at = jnp.where(odd == 1, ring - 1 - row // 2, row // 2)

    def row_at(p):
        p = lax.rem(p + ring, ring)
        return jnp.where(p < ring // 2, 2 * p, 2 * (ring - 1 - p) + 1)

    targets = (row_at(at + 1), row_at(at - 1))
    place = (at, lax.rem(ring - at, ring))
    has_up, has_down = row > 0, row < ring - 1

    barrier = pltpu.get_barrier_semaphore()

    def greet(r, c):
        pl.semaphore_signal(
            barrier, inc=1, device_id={"row": r, "col": c}, device_id_type=MESH
        )

    greet(row, 1 - col)
    greet(targets[0], col)
    greet(targets[1], col)

    @pl.when(has_up)
    def _():
        greet(row - 1, col)

    @pl.when(has_down)
    def _():
        greet(row + 1, col)

    pl.semaphore_wait(barrier, 3 + jnp.where(has_up, 1, 0) + jnp.where(has_down, 1, 0))

    def remote(src, dst, s, r, to_row, to_col):
        return pltpu.make_async_remote_copy(
            src_ref=src, dst_ref=dst, send_sem=s, recv_sem=r,
            device_id={"row": to_row, "col": to_col}, device_id_type=MESH,
        )

    first = remote(grad.at[1 - mine], other, core_s.at[0], core_r.at[0], row, 1 - col)
    first.start()
    peak_first = remote(peak, peaks.at[0], pk_s.at[0], pk_r.at[0], row, 1 - col)
    peak_first.start()
    numer_copy = remote(numer, mate, core_s.at[1], core_r.at[1], row, 1 - col)
    numer_copy.start()
    up = remote(
        numer.at[:, pl.ds(0, half), :], rims.at[mine, 1], rim_s.at[0], rim_r.at[1],
        row - 1, col,
    )
    down = remote(
        numer.at[:, pl.ds(half, half), :], rims.at[mine, 0], rim_s.at[1], rim_r.at[0],
        row + 1, col,
    )

    @pl.when(has_up)
    def _():
        up.start()

    @pl.when(has_down)
    def _():
        down.start()

    def spot(k, d, u):
        k = lax.rem(k + 2 * ring, ring)
        start = (k * 2 + d) * chunk + pieces[u][0]
        return pl.ds(pl.multiple_of(start, 8), pieces[u][1])

    def box(d, u):
        return pl.ds(d * chunk + pieces[u][0], pieces[u][1])

    streams = [(d, u) for u in range(len(pieces)) for d in range(2)]

    def rs_copy(src, s, d, u):
        return remote(
            src, inbox.at[s, box(d, u), :], rs_s.at[s, d, u], rs_r.at[s, d, u], targets[d], col
        )

    def ag_copy(s, d, u):
        here = total.at[mine, spot(place[d] + 1 - s, d, u), :]
        return remote(here, here, ag_s.at[s, d, u], ag_r.at[s, d, u], targets[d], col)

    def dd_copy(s, d, u):
        here = total.at[mine, spot(place[d] + 1 - s, d, u), :]
        return remote(here, here, dd_s.at[s, d, u], dd_r.at[s, d, u], row, 1 - col)

    def pk_copy(src, s):
        return remote(src, peaks.at[s + 1], pk_s.at[s + 1], pk_r.at[s + 1], targets[0], col)

    peak_first.wait()
    top[...] = jnp.maximum(peak[...], peaks[0])
    pk_copy(top, 0).start()
    first.wait()
    own[...] = grad[mine] + other[...]
    for d, u in streams:
        rs_copy(own.at[spot(place[d], d, u), :], 0, d, u).start()

    def scatter_step(s, carry):
        pk_copy(top, s).wait_recv()
        peaks[s + 1] = jnp.maximum(peaks[s + 1], top[...])
        pk_copy(peaks.at[s + 1], s + 1).start()
        for d, u in streams:
            rs_copy(own.at[spot(0, d, u), :], s, d, u).wait_recv()
            inbox[s, box(d, u), :] += own[spot(place[d] - s - 1, d, u), :]
            rs_copy(inbox.at[s, box(d, u), :], s + 1, d, u).start()
        return carry

    lax.fori_loop(0, ring - 2, scatter_step, 0)
    last = ring - 2
    for d, u in streams:
        rs_copy(own.at[spot(0, d, u), :], last, d, u).wait_recv()
        here = spot(place[d] + 1, d, u)
        total[mine, here, :] = inbox[last, box(d, u), :] + own[here, :]
        ag_copy(0, d, u).start()
        dd_copy(0, d, u).start()
    pk_copy(top, last).wait_recv()

    fwd = [
        remote(rims.at[mine, t], rims.at[mine, t], fwd_s.at[t], fwd_r.at[t], row, 1 - col)
        for t in range(2)
    ]

    @pl.when(has_down)
    def _():
        remote(
            numer.at[:, pl.ds(0, half), :], rims.at[mine, 1], rim_s.at[0], rim_r.at[1],
            row + 1, col,
        ).wait_recv()
        fwd[1].start()

    @pl.when(has_up)
    def _():
        remote(
            numer.at[:, pl.ds(half, half), :], rims.at[mine, 0], rim_s.at[1], rim_r.at[0],
            row - 1, col,
        ).wait_recv()
        fwd[0].start()

    def gather_step(s, carry):
        for d, u in streams:
            ag_copy(s, d, u).wait_recv()

            @pl.when(s < ring - 2)
            def _():
                ag_copy(s + 1, d, u).start()

            dd_copy(s + 1, d, u).start()
        return carry

    lax.fori_loop(0, ring - 1, gather_step, 0)

    def finish(s, carry):
        for d, u in streams:
            rs_copy(own.at[spot(0, d, u), :], s, d, u).wait_send()
            ag_copy(s, d, u).wait_send()
            dd_copy(s, d, u).wait()
        pk_copy(top, s).wait_send()
        return carry

    lax.fori_loop(0, ring - 1, finish, 0)
    for d, u in streams:
        dd_copy(ring - 1, d, u).wait()
    numer_copy.wait()

    @pl.when(has_up)
    def _():
        up.wait_send()
        fwd[0].wait()

    @pl.when(has_down)
    def _():
        down.wait_send()
        fwd[1].wait()

    top[...] = jnp.maximum(peaks[ring - 1], top[...])


def object_kernel(places, here, obj, numer, mate, rims, illum, top, out, acc):
    tile_rows, tile_cols = illum.shape
    side = numer.shape[2]
    half = side // 2
    mine = here[0]
    acc[...] = jnp.zeros_like(acc)

    def put(block, start, k):
        valid = places[k, 2]
        block = jnp.where(valid != 0, block, 0.0)
        rh, rl = split(block[0])
        ih, il = split(block[1])
        stacked = cat([rh, ih, rl, il], 1)
        picked = dot(row_picker(tile_rows, block.shape[1], start, valid), stacked).astype(BF16)
        tall = cat([picked[:, i * side : (i + 1) * side] for i in range(4)], 0)
        acc[...] += dot(tall, col_picker(side, tile_cols, places[k, 1]))

    for c in range(2):
        put(jnp.where(mine == c, numer[...], mate[...]), places[2 + c, 0], 2 + c)
        put(rims[c, 0], places[c, 0] + half, c)
        put(rims[c, 1], places[4 + c, 0], 4 + c)
    scale = 1.0 / (illum[...] + 0.1 * jnp.max(top[...]))
    for t in range(2):
        high = acc[t * tile_rows : (t + 1) * tile_rows]
        low = acc[(2 + t) * tile_rows : (3 + t) * tile_rows]
        out[t] = obj[t] + (high + low) * scale


def probe_kernel(probe, total, out):
    modes, side = probe.shape[1], probe.shape[2]
    half = side // 2
    top = 2 * modes * half
    biggest = jnp.max(
        jnp.maximum(total[0, top : top + half, :], total[1, top : top + half, :])
    )
    for t in range(2):
        scale = 1.0 / (total[t, top : top + half, :] + 0.1 * biggest)
        for i in range(2):
            for m in range(modes):
                line = (i * modes + m) * half
                out[i, m, t * half : (t + 1) * half, :] = (
                    probe[i, m, t * half : (t + 1) * half, :].astype(F32)
                    + total[t, line : line + half, :] * scale
                )


def struct(shape, kind=F32):
    return jax.ShapeDtypeStruct(shape, kind)


def local(obj_field, probe_modes, centers, amplitudes):
    tile_rows, tile_cols = obj_field.shape[1:]
    modes, side = probe_modes.shape[1:3]
    margin = side // 2
    ring, cores = lax.axis_size("row"), lax.axis_size("col")
    row, col = lax.axis_index("row"), lax.axis_index("col")
    origin = jnp.stack([row * tile_rows, col * tile_cols]).astype(jnp.int32)

    extended = padded(obj_field, (("row", 1), ("col", 2)), margin)
    near = padded(centers.reshape(1, 1, 2), (("row", 0),), 1)
    mate_list = lax.ppermute(near, "col", [(0, 1), (1, 0)])
    listed = jnp.where(
        col == 0, jnp.concatenate([near, mate_list], 1), jnp.concatenate([mate_list, near], 1)
    ).reshape(3 * cores, 2)
    steps = jnp.arange(3 * cores, dtype=jnp.int32) // cores - 1 + row
    valid = ((steps >= 0) & (steps < ring)).astype(jnp.int32)
    places = jnp.concatenate([listed - margin - origin, valid[:, None]], 1)
    start = centers[0] - origin
    window = lax.dynamic_slice(extended, (0, start[0], start[1]), (2, side, side))

    lines = (2 * modes + 1) * margin
    chunk, pieces = ring_split(lines, ring)
    depth = 2 * ring * chunk
    count = len(pieces)
    params = pltpu.CompilerParams(vmem_limit_bytes=LIMIT)
    grad, numer, illum, peak = pl.pallas_call(
        update_kernel,
        out_shape=(
            struct((2, depth, side)),
            struct((2, side, side)),
            struct((tile_rows, tile_cols)),
            struct((8, 128)),
        ),
        in_specs=[SMEM] + [VMEM] * 8,
        out_specs=(VMEM,) * 4,
        scratch_shapes=[
            pltpu.VMEM((2, modes, side, side), F32),
            pltpu.VMEM((2, side, side), F32),
        ],
        compiler_params=params,
        name="update",
    )(places, window, probe_modes, amplitudes[0], *tables(side))

    dma = pltpu.SemaphoreType.DMA
    total, rims, mate, top = pl.pallas_call(
        functools.partial(exchange_kernel, ring, chunk, pieces),
        out_shape=(
            struct((2, depth, side)),
            struct((2, 2, 2, margin, side)),
            struct((2, side, side)),
            struct((8, 128)),
        ),
        in_specs=[VMEM] * 3,
        out_specs=(VMEM,) * 4,
        scratch_shapes=[
            pltpu.VMEM((depth, side), F32),
            pltpu.VMEM((ring - 1, 2 * chunk, side), F32),
            pltpu.VMEM((depth, side), F32),
            pltpu.VMEM((ring, 8, 128), F32),
            dma((2,)), dma((2,)),
            dma((ring - 1, 2, count)), dma((ring - 1, 2, count)),
            dma((ring - 1, 2, count)), dma((ring - 1, 2, count)),
            dma((ring, 2, count)), dma((ring, 2, count)),
            dma((2,)), dma((2,)), dma((2,)), dma((2,)),
            dma((ring,)), dma((ring,)),
        ],
        compiler_params=pltpu.CompilerParams(
            vmem_limit_bytes=LIMIT, collective_id=1, has_side_effects=True
        ),
        name="exchange",
    )(grad, numer, peak)

    new_object = pl.pallas_call(
        object_kernel,
        out_shape=struct(obj_field.shape),
        in_specs=[SMEM, SMEM] + [VMEM] * 6,
        out_specs=VMEM,
        scratch_shapes=[pltpu.VMEM((4 * tile_rows, tile_cols), F32)],
        compiler_params=params,
        name="object",
    )(places, col.reshape(1).astype(jnp.int32), obj_field, numer, mate, rims, illum, top)
    new_probe = pl.pallas_call(
        probe_kernel,
        out_shape=struct(probe_modes.shape),
        in_specs=[VMEM] * 2,
        out_specs=VMEM,
        compiler_params=params,
        name="probe",
    )(probe_modes, total)
    return (new_object, new_probe)


def solution(mesh):
    in_specs = (
        P(None, ("angle", "row"), "col"),
        P(),
        P(("angle", "row", "col"), None),
        P(("angle", "row", "col"), None, None),
    )
    out_specs = (P(None, ("angle", "row"), "col"), P(None, "angle", None, None))
    return jax.shard_map(local, mesh=mesh, in_specs=in_specs, out_specs=out_specs, check_vma=False)
```

```python
import functools
import math

import jax
import jax.numpy as jnp
import numpy as np
from jax import lax
from jax.experimental import pallas as pl
from jax.experimental.pallas import tpu as pltpu
from jax.sharding import PartitionSpec as P

MESH = pl.DeviceIdType.MESH
F32 = jnp.float32
BF16 = jnp.bfloat16
VMEM = pl.BlockSpec(memory_space=pltpu.VMEM)
SMEM = pl.BlockSpec(memory_space=pltpu.SMEM)
LIMIT = 60 * 1024 * 1024


def split(x):
    high = x.astype(BF16)
    return high, (x - high.astype(F32)).astype(BF16)


def dot(a, b):
    return jnp.dot(a, b, preferred_element_type=F32)


def dot3(a, b):
    return dot(a[0], b[1]) + dot(a[1], b[0]) + dot(a[0], b[0])


def tables(side):
    half = side // 2
    k = np.arange(half)
    phase = (k[:, None] * k[None, :] % half) * (2.0 * math.pi / half)
    scale = 1.0 / math.sqrt(side)
    cosine, sine = np.cos(phase) * scale, np.sin(phase) * scale
    matrix = np.block([[cosine, sine], [-sine, cosine]]).astype(np.float32)
    turn = k * (2.0 * math.pi / side)
    lanes = np.stack([np.cos(turn), np.sin(turn)]).astype(np.float32)
    rows = np.broadcast_to(lanes[:, :, None], (2, half, side))
    order = np.concatenate([np.arange(0, side, 2), np.arange(1, side, 2)])
    shuffle = (np.arange(side)[:, None] == order[None, :]).astype(np.float32)
    high = matrix.astype(BF16)
    low = (matrix - high.astype(np.float32)).astype(BF16)
    return (
        jnp.asarray(np.stack([high, low])),
        jnp.asarray(np.stack([high.T, low.T])),
        jnp.asarray(rows),
        jnp.asarray(lanes),
        jnp.asarray(np.stack([shuffle, shuffle.T])).astype(BF16),
    )


def cat(parts, axis):
    return jnp.concatenate(parts, axis=axis)


def forward_transform(re, im, a, b, rows, lanes):
    h = re.shape[0] // 2
    n = 2 * h
    er, ei = re[:h] + re[h:], im[:h] + im[h:]
    dr, di = re[:h] - re[h:], im[:h] - im[h:]
    c, s = rows
    stacked = cat([cat([er, dr * c + di * s], 1), cat([ei, di * c - dr * s], 1)], 0)
    y = dot3(a, split(stacked))
    yr = cat([y[:h, :n], y[:h, n:]], 0)
    yi = cat([y[h:, :n], y[h:, n:]], 0)
    er, ei = yr[:, :h] + yr[:, h:], yi[:, :h] + yi[:, h:]
    dr, di = yr[:, :h] - yr[:, h:], yi[:, :h] - yi[:, h:]
    c, s = lanes
    stacked = cat([cat([er, ei], 1), cat([dr * c + di * s, di * c - dr * s], 1)], 0)
    z = dot3(split(stacked), b)
    return cat([z[:n, :h], z[n:, :h]], 1), cat([z[:n, h:], z[n:, h:]], 1)


def inverse_transform(fr, fi, a, b, rows, lanes):
    h = fr.shape[0] // 2
    n = 2 * h
    stacked = cat([cat([fr[:, :h], fi[:, :h]], 1), cat([fr[:, h:], fi[:, h:]], 1)], 0)
    z = dot3(split(stacked), a)
    er, ei, odr, odi = z[:n, :h], z[:n, h:], z[n:, :h], z[n:, h:]
    c, s = lanes
    tr, ti = odr * c - odi * s, odi * c + odr * s
    yr = cat([er + tr, er - tr], 1)
    yi = cat([ei + ti, ei - ti], 1)
    stacked = cat([cat([yr[:h], yr[h:]], 1), cat([yi[:h], yi[h:]], 1)], 0)
    v = dot3(b, split(stacked))
    er, ei, odr, odi = v[:h, :n], v[h:, :n], v[:h, n:], v[h:, n:]
    c, s = rows
    tr, ti = odr * c - odi * s, odi * c + odr * s
    return cat([er + tr, er - tr], 0), cat([ei + ti, ei - ti], 0)


def row_picker(count, depth, start, valid):
    place = lax.broadcasted_iota(jnp.int32, (count, depth), 0) - lax.broadcasted_iota(
        jnp.int32, (count, depth), 1
    )
    return jnp.where(place == start, valid, 0.0).astype(BF16)


def col_picker(depth, count, start):
    place = lax.broadcasted_iota(jnp.int32, (depth, count), 1) - lax.broadcasted_iota(
        jnp.int32, (depth, count), 0
    )
    return jnp.where(place == start, 1.0, 0.0).astype(BF16)


def corner(known, k, tile_rows, tile_cols, margin):
    row, col = lax.axis_index("row"), lax.axis_index("col")
    line = row + k // 2 - 1
    inside = (line >= 0) & (line < lax.axis_size("row"))
    mark = known[k]
    return (
        mark[0:1, 0:1] - (row * tile_rows + margin),
        mark[1:2, 0:1] - (col * tile_cols + margin),
        jnp.where(inside, 1.0, 0.0),
    )


def update_kernel(
    center, known, column, probe, amp, a_ref, b_ref, rows_ref, lanes_ref, shuffle,
    grad, numer, illum, peak, far, power, window,
):
    modes, side = probe.shape[1], probe.shape[2]
    half = side // 2
    a = (a_ref[0], a_ref[1])
    b = (b_ref[0], b_ref[1])
    rows = (rows_ref[0], rows_ref[1])
    lanes = (lanes_ref[0:1, :], lanes_ref[1:2, :])

    def wave(m):
        pr, pi = probe[0, m].astype(F32), probe[1, m].astype(F32)
        wr, wi = window[0], window[1]
        return pr, pi, wr, wi, pr * wr - pi * wi, pr * wi + pi * wr

    start = center[0, 0] - lax.axis_index("row") * illum.shape[0]
    base = pl.multiple_of(start // 8 * 8, 8)
    shift = lax.rem(side + 8 - lax.rem(start, 8), side + 8)
    for i in range(2):
        window[i] = pltpu.roll(column[i, pl.ds(base, side + 8), :], shift, 0)[:side]
    power[...] = jnp.zeros_like(power)

    def ahead(m, carry):
        pr, pi, wr, wi, xr, xi = wave(m)
        fr, fi = forward_transform(xr, xi, a, b, rows, lanes)
        far[0, m] = fr
        far[1, m] = fi
        power[0] += fr * fr + fi * fi
        power[1] += pr * pr + pi * pi
        return carry

    lax.fori_loop(0, modes, ahead, 0)
    measured = 0.0
    rest = amp[...]
    for i in range(3):
        piece = rest.astype(BF16)
        rest = rest - piece.astype(F32)
        measured += dot(dot(shuffle[1], piece).astype(BF16), shuffle[0])
    power[0] = measured / (jnp.sqrt(power[0]) + 0.5)
    high, low = split(power[1])
    tile_rows, tile_cols = illum.shape
    spot = cat([high, low], 1)
    illum[...] = jnp.zeros_like(illum)

    def place_spot(k, carry):
        top, left, valid = corner(known, k, tile_rows, tile_cols, half)
        picked = dot(row_picker(tile_rows, side, top, valid), spot).astype(BF16)
        across = col_picker(side, tile_cols, left)
        placed = dot(cat([picked[:, :side], picked[:, side:]], 0), across)
        illum[...] += placed[:tile_rows] + placed[tile_rows:]
        return carry

    lax.fori_loop(0, known.shape[0], place_spot, 0)
    peak[...] = jnp.full(peak.shape, jnp.max(illum[...]), F32)
    numer[...] = jnp.zeros_like(numer)

    def back(m, carry):
        pr, pi, wr, wi, xr, xi = wave(m)
        factor = power[0]
        gr, gi = inverse_transform(far[0, m] * factor, far[1, m] * factor, a, b, rows, lanes)
        dr, di = gr - xr, gi - xi
        numer[0] += pr * dr + pi * di
        numer[1] += pr * di - pi * dr
        ur = wr * dr + wi * di
        ui = wr * di - wi * dr
        for t in range(2):
            grad[t, pl.ds(pl.multiple_of(m * half, half), half), :] = ur[t * half : (t + 1) * half]
            grad[t, pl.ds(pl.multiple_of((modes + m) * half, half), half), :] = ui[
                t * half : (t + 1) * half
            ]
        return carry

    lax.fori_loop(0, modes, back, 0)
    weight = window[0] * window[0] + window[1] * window[1]
    top = 2 * modes * half
    for t in range(2):
        grad[t, top : top + half, :] = weight[t * half : (t + 1) * half]
        if grad.shape[1] > top + half:
            grad[t, top + half :, :] = jnp.zeros((grad.shape[1] - top - half, side), F32)


def gather_kernel(
    ring, marks, obj, column, known,
    strip, packed, near_s, near_r, tile_s, tile_r, pack_s, pack_r, pass_s, pass_r,
):
    row, col = lax.axis_index("row"), lax.axis_index("col")
    tile_rows, tile_cols = obj.shape[1:]
    side = column.shape[2]
    half = side // 2
    has = (row > 0, row < ring - 1)
    beside = (row - 1, row + 1)
    barrier = pltpu.get_barrier_semaphore()

    def greet(r, c):
        pl.semaphore_signal(
            barrier, inc=1, device_id={"row": r, "col": c}, device_id_type=MESH
        )

    greet(row, 1 - col)
    for t in range(2):

        @pl.when(has[t])
        def _():
            greet(beside[t], col)

    pl.semaphore_wait(barrier, 1 + jnp.where(has[0], 1, 0) + jnp.where(has[1], 1, 0))

    def remote(src, dst, s, r, to_row, to_col):
        return pltpu.make_async_remote_copy(
            src_ref=src, dst_ref=dst, send_sem=s, recv_sem=r,
            device_id={"row": to_row, "col": to_col}, device_id_type=MESH,
        )

    def own_lanes(c):
        return pl.ds(pl.multiple_of(half + c * tile_cols, 128), tile_cols)

    near = [
        remote(marks, known.at[2 * (1 - t), col], near_s.at[t], near_r.at[1 - t], beside[t], col)
        for t in range(2)
    ]
    mate_mark = remote(marks, known.at[1, col], near_s.at[2], near_r.at[2], row, 1 - col)
    tile = remote(obj, strip.at[:, :, own_lanes(col)], tile_s, tile_r, row, 1 - col)
    for t in range(2):

        @pl.when(has[t])
        def _():
            near[t].start()

    tile.start()
    mate_mark.start()
    strip[:, :, :half] = jnp.zeros((2, tile_rows, half), F32)
    strip[:, :, half + 2 * tile_cols :] = jnp.zeros((2, tile_rows, half), F32)
    strip[:, :, own_lanes(col)] = obj[...]
    tile.wait()

    def cut(mark):
        width = strip.shape[2]
        place = lax.broadcasted_iota(jnp.int32, (width, side), 0) - lax.broadcasted_iota(
            jnp.int32, (width, side), 1
        )
        pick = jnp.where(place == mark[1:2, 0:1], 1.0, 0.0).astype(BF16)
        rest, found = strip[...].reshape(2 * tile_rows, width), 0.0
        for _ in range(3):
            piece = rest.astype(BF16)
            rest = rest - piece.astype(F32)
            found += dot(piece, pick)
        return found.reshape(2, tile_rows, side)

    def pack(t):
        return remote(
            packed.at[t], column.at[:, pl.ds(2 * (1 - t) * tile_rows, tile_rows), :],
            pack_s.at[t], pack_r.at[1 - t], beside[t], col,
        )

    def arrived_pack(t):
        return remote(
            packed.at[1 - t], column.at[:, pl.ds(2 * t * tile_rows, tile_rows), :],
            pack_s.at[1 - t], pack_r.at[t], beside[t], col,
        )

    def share(t):
        here = known.at[2 * t, col]
        return remote(here, here, pass_s.at[t], pass_r.at[t], row, 1 - col)

    for t in range(2):

        @pl.when(has[t])
        def _():
            remote(
                marks, known.at[2 * t, col], near_s.at[1 - t], near_r.at[t], beside[t], col
            ).wait_recv()
            share(t).start()
            packed[t] = cut(known[2 * t, col])
            pack(t).start()

    known[1, col] = marks[...]
    column[:, tile_rows : 2 * tile_rows, :] = cut(marks[...])
    for t in range(2):

        @pl.when(jnp.logical_not(has[t]))
        def _():
            column[:, 2 * t * tile_rows : (2 * t + 1) * tile_rows, :] = jnp.zeros(
                (2, tile_rows, side), F32
            )

    mate_mark.wait()
    for t in range(2):

        @pl.when(has[t])
        def _():
            share(t).wait()

    for t in range(2):

        @pl.when(has[t])
        def _():
            pack(t).wait_send()
            remote(
                marks, known.at[2 * (1 - t), col], near_s.at[t], near_r.at[1 - t], beside[t], col
            ).wait_send()
            arrived_pack(t).wait_recv()


def ring_split(lines, ring):
    chunk = -(-lines // (16 * ring)) * 8
    pieces = min(2, chunk // 8)
    offsets, at = [], 0
    for i in range(pieces):
        size = (chunk // 8 // pieces + (1 if i < chunk // 8 % pieces else 0)) * 8
        offsets.append((at, size))
        at += size
    return chunk, offsets


def exchange_kernel(
    ring, chunk, pieces, grad, numer, peak, total, rims, mate, top,
    own, inbox, other, seen, highs, core_s, core_r, rs_s, rs_r, ag_s, ag_r, dd_s, dd_r,
    mine_s, mine_r, rim_s, rim_r, fwd_s, fwd_r, pk_s, pk_r,
):
    row, col = lax.axis_index("row"), lax.axis_index("col")
    side = grad.shape[2]
    half = side // 2
    mine = col
    odd = lax.rem(row, 2)
    at = jnp.where(odd == 1, ring - 1 - row // 2, row // 2)

    def row_at(p):
        p = lax.rem(p + ring, ring)
        return jnp.where(p < ring // 2, 2 * p, 2 * (ring - 1 - p) + 1)

    targets = (row_at(at + 1), row_at(at - 1))
    place = (at, lax.rem(ring - at, ring))
    has_up, has_down = row > 0, row < ring - 1

    barrier = pltpu.get_barrier_semaphore()

    def greet(r, c):
        pl.semaphore_signal(
            barrier, inc=1, device_id={"row": r, "col": c}, device_id_type=MESH
        )

    greet(row, 1 - col)
    greet(targets[0], col)
    greet(targets[1], col)

    @pl.when(has_up)
    def _():
        greet(row - 1, col)

    @pl.when(has_down)
    def _():
        greet(row + 1, col)

    pl.semaphore_wait(barrier, 3 + jnp.where(has_up, 1, 0) + jnp.where(has_down, 1, 0))

    def remote(src, dst, s, r, to_row, to_col):
        return pltpu.make_async_remote_copy(
            src_ref=src, dst_ref=dst, send_sem=s, recv_sem=r,
            device_id={"row": to_row, "col": to_col}, device_id_type=MESH,
        )

    first = remote(grad.at[1 - mine], other, core_s.at[0], core_r.at[0], row, 1 - col)
    first.start()
    peak_first = remote(peak, top, core_s.at[2], core_r.at[2], row, 1 - col)
    peak_first.start()
    numer_copy = remote(numer, mate, core_s.at[1], core_r.at[1], row, 1 - col)
    numer_copy.start()
    up = remote(
        numer.at[:, pl.ds(0, half), :], rims.at[mine, 1], rim_s.at[0], rim_r.at[1],
        row - 1, col,
    )
    down = remote(
        numer.at[:, pl.ds(half, half), :], rims.at[mine, 0], rim_s.at[1], rim_r.at[0],
        row + 1, col,
    )

    @pl.when(has_up)
    def _():
        up.start()

    @pl.when(has_down)
    def _():
        down.start()

    far = ring // 2

    def reach(b, d):
        return far if b == d else far - 1

    def spot(q, b, d, u):
        k = lax.rem(q + 2 * ring, ring)
        if d == 1:
            k = lax.rem(ring - k, ring)
        start = (k * 2 + b) * chunk + pieces[u][0]
        return pl.ds(pl.multiple_of(start, 8), pieces[u][1])

    def box(b, d, u):
        return pl.ds((2 * b + d) * chunk + pieces[u][0], pieces[u][1])

    flows = [(b, d, u) for u in range(len(pieces)) for b in range(2) for d in range(2)]

    def rs_copy(src, s, b, d, u):
        return remote(
            src, inbox.at[s, box(b, d, u), :], rs_s.at[s, b, d, u], rs_r.at[s, b, d, u],
            targets[d], col,
        )

    def rs_wait(s, b, d, u):
        return rs_copy(inbox.at[s, box(b, d, u), :], s, b, d, u)

    def ag_copy(s, b, d, u):
        here = total.at[mine, spot(place[d] - s, b, d, u), :]
        return remote(
            here, here, ag_s.at[s, b, d, u], ag_r.at[s, b, d, u], targets[d], col
        )

    def dd_copy(s, b, d, u):
        here = total.at[mine, spot(place[d] - 1 - s, b, d, u), :]
        return remote(here, here, dd_s.at[s, b, d, u], dd_r.at[s, b, d, u], row, 1 - col)

    def mine_copy(b, u):
        here = total.at[mine, spot(at, b, 0, u), :]
        return remote(here, here, mine_s.at[b, u], mine_r.at[b, u], row, 1 - col)

    def pk_copy(s, d):
        return remote(
            highs.at[s], seen.at[s, d], pk_s.at[s, d], pk_r.at[s, d], targets[d], col
        )

    peak_first.wait()
    highs[0] = jnp.maximum(peak[...], top[...])
    for d in range(2):
        pk_copy(0, d).start()
    first.wait()
    own[...] = grad[mine] + other[...]
    for b, d, u in flows:
        rs_copy(own.at[spot(place[d] + reach(b, d), b, d, u), :], 0, b, d, u).start()

    def pass_on(s, b, d, u):
        inbox[s, box(b, d, u), :] += own[spot(place[d] + reach(b, d) - s - 1, b, d, u), :]
        rs_copy(inbox.at[s, box(b, d, u), :], s + 1, b, d, u).start()

    def pass_peak(s):
        for d in range(2):
            pk_copy(s, d).wait_recv()
        highs[s + 1] = jnp.maximum(highs[s], jnp.maximum(seen[s, 0], seen[s, 1]))

    def scatter_step(s, carry):
        pass_peak(s)
        for d in range(2):
            pk_copy(s + 1, d).start()
        for b, d, u in flows:
            rs_wait(s, b, d, u).wait_recv()
            pass_on(s, b, d, u)
        return carry

    lax.fori_loop(0, far - 2, scatter_step, 0)
    pass_peak(far - 2)
    for d in range(2):
        pk_copy(far - 1, d).start()
    for b, d, u in flows:
        rs_wait(far - 2, b, d, u).wait_recv()
        if b == d:
            pass_on(far - 2, b, d, u)
    for u in range(len(pieces)):
        for b in range(2):
            rs_wait(far - 1, b, b, u).wait_recv()
            here = spot(at, b, 0, u)
            total[mine, here, :] = (
                own[here, :] + inbox[far - 1, box(b, b, u), :] + inbox[far - 2, box(b, 1 - b, u), :]
            )
            for d in range(2):
                ag_copy(0, b, d, u).start()
            mine_copy(b, u).start()
    pass_peak(far - 1)

    fwd = [
        remote(rims.at[mine, t], rims.at[mine, t], fwd_s.at[t], fwd_r.at[t], row, 1 - col)
        for t in range(2)
    ]

    @pl.when(has_down)
    def _():
        remote(
            numer.at[:, pl.ds(0, half), :], rims.at[mine, 1], rim_s.at[0], rim_r.at[1],
            row + 1, col,
        ).wait_recv()
        fwd[1].start()

    @pl.when(has_up)
    def _():
        remote(
            numer.at[:, pl.ds(half, half), :], rims.at[mine, 0], rim_s.at[1], rim_r.at[0],
            row - 1, col,
        ).wait_recv()
        fwd[0].start()

    def gather_step(s, carry):
        for b, d, u in flows:
            ag_copy(s, b, d, u).wait_recv()
            ag_copy(s + 1, b, d, u).start()
            dd_copy(s, b, d, u).start()
        return carry

    lax.fori_loop(0, far - 2, gather_step, 0)
    for b, d, u in flows:
        ag_copy(far - 2, b, d, u).wait_recv()
        if b == d:
            ag_copy(far - 1, b, d, u).start()
        dd_copy(far - 2, b, d, u).start()
    for b, d, u in flows:
        if b == d:
            ag_copy(far - 1, b, d, u).wait_recv()
            dd_copy(far - 1, b, d, u).start()

    def settle(s, b, d, u):
        rs_wait(s, b, d, u).wait_send()
        ag_copy(s, b, d, u).wait_send()
        dd_copy(s, b, d, u).wait()

    def finish(s, carry):
        for b, d, u in flows:
            settle(s, b, d, u)
        for d in range(2):
            pk_copy(s, d).wait_send()
        return carry

    lax.fori_loop(0, far - 1, finish, 0)
    for b, d, u in flows:
        if b == d:
            settle(far - 1, b, d, u)
    for d in range(2):
        pk_copy(far - 1, d).wait_send()
    for u in range(len(pieces)):
        for b in range(2):
            mine_copy(b, u).wait()
    numer_copy.wait()

    @pl.when(has_up)
    def _():
        up.wait_send()
        fwd[0].wait()

    @pl.when(has_down)
    def _():
        down.wait_send()
        fwd[1].wait()

    top[...] = highs[far]


def object_kernel(known, obj, numer, mate, rims, illum, top, out, acc):
    tile_rows, tile_cols = illum.shape
    side = numer.shape[2]
    half = side // 2
    mine = lax.axis_index("col")
    acc[...] = jnp.zeros_like(acc)

    def put(block, offset, k):
        top, left, valid = corner(known, k, tile_rows, tile_cols, half)
        block = jnp.where(valid > 0.0, block, 0.0)
        rh, rl = split(block[0])
        ih, il = split(block[1])
        stacked = cat([rh, ih, rl, il], 1)
        pick = row_picker(tile_rows, block.shape[1], top + offset, valid)
        picked = dot(pick, stacked).astype(BF16)
        tall = cat([picked[:, i * side : (i + 1) * side] for i in range(4)], 0)
        acc[...] += dot(tall, col_picker(side, tile_cols, left))

    for c in range(2):
        put(jnp.where(mine == c, numer[...], mate[...]), 0, 2 + c)
        put(rims[c, 0], half, c)
        put(rims[c, 1], 0, 4 + c)
    scale = 1.0 / (illum[...] + 0.1 * jnp.max(top[...]))
    for t in range(2):
        high = acc[t * tile_rows : (t + 1) * tile_rows]
        low = acc[(2 + t) * tile_rows : (3 + t) * tile_rows]
        out[t] = obj[t] + (high + low) * scale


def probe_kernel(probe, total, out):
    modes, side = probe.shape[1], probe.shape[2]
    half = side // 2
    top = 2 * modes * half
    biggest = jnp.max(
        jnp.maximum(total[0, top : top + half, :], total[1, top : top + half, :])
    )
    for t in range(2):
        scale = 1.0 / (total[t, top : top + half, :] + 0.1 * biggest)
        for i in range(2):
            for m in range(modes):
                line = (i * modes + m) * half
                out[i, m, t * half : (t + 1) * half, :] = (
                    probe[i, m, t * half : (t + 1) * half, :].astype(F32)
                    + total[t, line : line + half, :] * scale
                )


def struct(shape, kind=F32):
    return jax.ShapeDtypeStruct(shape, kind)


def local(obj_field, probe_modes, centers, amplitudes):
    tile_rows, tile_cols = obj_field.shape[1:]
    modes, side = probe_modes.shape[1:3]
    margin = side // 2
    ring, cores = lax.axis_size("row"), lax.axis_size("col")
    dma = pltpu.SemaphoreType.DMA
    marks = jnp.broadcast_to(jnp.tile(centers[0], 4)[:, None], (8, 128))
    column, known = pl.pallas_call(
        functools.partial(gather_kernel, ring),
        out_shape=(struct((2, 3 * tile_rows, side)), struct((3, cores, 8, 128), jnp.int32)),
        in_specs=[VMEM, VMEM],
        out_specs=(VMEM, VMEM),
        scratch_shapes=[
            pltpu.VMEM((2, tile_rows, cores * tile_cols + side), F32),
            pltpu.VMEM((2, 2, tile_rows, side), F32),
            dma((3,)), dma((3,)), dma, dma, dma((2,)), dma((2,)), dma((2,)), dma((2,)),
        ],
        compiler_params=pltpu.CompilerParams(
            vmem_limit_bytes=LIMIT, collective_id=2, has_side_effects=True
        ),
        name="gather",
    )(marks, obj_field)
    known = known.reshape(3 * cores, 8, 128)

    lines = (2 * modes + 1) * margin
    chunk, pieces = ring_split(lines, ring)
    depth = 2 * ring * chunk
    count = len(pieces)
    params = pltpu.CompilerParams(vmem_limit_bytes=LIMIT)
    grad, numer, illum, peak = pl.pallas_call(
        update_kernel,
        out_shape=(
            struct((2, depth, side)),
            struct((2, side, side)),
            struct((tile_rows, tile_cols)),
            struct((8, 128)),
        ),
        in_specs=[SMEM] + [VMEM] * 9,
        out_specs=(VMEM,) * 4,
        scratch_shapes=[
            pltpu.VMEM((2, modes, side, side), F32),
            pltpu.VMEM((2, side, side), F32),
            pltpu.VMEM((2, side, side), F32),
        ],
        compiler_params=params,
        name="update",
    )(centers, known, column, probe_modes, amplitudes[0], *tables(side))

    total, rims, mate, top = pl.pallas_call(
        functools.partial(exchange_kernel, ring, chunk, pieces),
        out_shape=(
            struct((2, depth, side)),
            struct((2, 2, 2, margin, side)),
            struct((2, side, side)),
            struct((8, 128)),
        ),
        in_specs=[VMEM] * 3,
        out_specs=(VMEM,) * 4,
        scratch_shapes=[
            pltpu.VMEM((depth, side), F32),
            pltpu.VMEM((ring // 2, 4 * chunk, side), F32),
            pltpu.VMEM((depth, side), F32),
            pltpu.VMEM((ring // 2, 2, 8, 128), F32),
            pltpu.VMEM((ring // 2 + 1, 8, 128), F32),
            dma((3,)), dma((3,)),
            *[dma((ring // 2, 2, 2, count))] * 6,
            dma((2, count)), dma((2, count)),
            dma((2,)), dma((2,)), dma((2,)), dma((2,)),
            dma((ring // 2, 2)), dma((ring // 2, 2)),
        ],
        compiler_params=pltpu.CompilerParams(
            vmem_limit_bytes=LIMIT, collective_id=1, has_side_effects=True
        ),
        name="exchange",
    )(grad, numer, peak)

    new_object = pl.pallas_call(
        object_kernel,
        out_shape=struct(obj_field.shape),
        in_specs=[VMEM] * 7,
        out_specs=VMEM,
        scratch_shapes=[pltpu.VMEM((4 * tile_rows, tile_cols), F32)],
        compiler_params=params,
        name="object",
    )(known, obj_field, numer, mate, rims, illum, top)
    new_probe = pl.pallas_call(
        probe_kernel,
        out_shape=struct(probe_modes.shape),
        in_specs=[VMEM] * 2,
        out_specs=VMEM,
        compiler_params=params,
        name="probe",
    )(probe_modes, total)
    return (new_object, new_probe)


def solution(mesh):
    in_specs = (
        P(None, ("angle", "row"), "col"),
        P(),
        P(("angle", "row", "col"), None),
        P(("angle", "row", "col"), None, None),
    )
    out_specs = (P(None, ("angle", "row"), "col"), P(None, "angle", None, None))
    return jax.shard_map(local, mesh=mesh, in_specs=in_specs, out_specs=out_specs, check_vma=False)
```

```python
import functools
import math

import jax
import jax.numpy as jnp
import numpy as np
from jax import lax
from jax.experimental import pallas as pl
from jax.experimental.pallas import tpu as pltpu
from jax.sharding import PartitionSpec as P

MESH = pl.DeviceIdType.MESH
F32 = jnp.float32
BF16 = jnp.bfloat16
VMEM = pl.BlockSpec(memory_space=pltpu.VMEM)
SMEM = pl.BlockSpec(memory_space=pltpu.SMEM)
LIMIT = 26 * 1024 * 1024


def split(x):
    high = x.astype(BF16)
    return high, (x - high.astype(F32)).astype(BF16)


def dot(a, b):
    return jnp.dot(a, b, preferred_element_type=F32)


def dot3(a, b):
    return dot(a[0], b[1]) + dot(a[1], b[0]) + dot(a[0], b[0])


def tables(side):
    half = side // 2
    k = np.arange(half)
    phase = (k[:, None] * k[None, :] % half) * (2.0 * math.pi / half)
    scale = 1.0 / math.sqrt(side)
    cosine, sine = np.cos(phase) * scale, np.sin(phase) * scale
    matrix = np.block([[cosine, sine], [-sine, cosine]]).astype(np.float32)
    turn = k * (2.0 * math.pi / side)
    lanes = np.stack([np.cos(turn), np.sin(turn)]).astype(np.float32)
    rows = np.ascontiguousarray(np.broadcast_to(lanes[:, :, None], (2, half, side)))
    order = np.concatenate([np.arange(0, side, 2), np.arange(1, side, 2)])
    shuffle = (np.arange(side)[:, None] == order[None, :]).astype(np.float32)
    high = matrix.astype(BF16)
    low = (matrix - high.astype(np.float32)).astype(BF16)
    return (
        jnp.asarray(np.stack([high, low])),
        jnp.asarray(np.stack([high.T, low.T])),
        jnp.asarray(rows),
        jnp.asarray(lanes),
        jnp.asarray(np.stack([shuffle, shuffle.T])).astype(BF16),
    )


def cat(parts, axis):
    return jnp.concatenate(parts, axis=axis)


def forward_transform(re, im, a, b, rows, lanes):
    h = re.shape[0] // 2
    n = 2 * h
    er, ei = re[:h] + re[h:], im[:h] + im[h:]
    dr, di = re[:h] - re[h:], im[:h] - im[h:]
    c, s = rows
    stacked = cat([cat([er, dr * c + di * s], 1), cat([ei, di * c - dr * s], 1)], 0)
    y = dot3(a, split(stacked))
    yr = cat([y[:h, :n], y[:h, n:]], 0)
    yi = cat([y[h:, :n], y[h:, n:]], 0)
    er, ei = yr[:, :h] + yr[:, h:], yi[:, :h] + yi[:, h:]
    dr, di = yr[:, :h] - yr[:, h:], yi[:, :h] - yi[:, h:]
    c, s = lanes
    stacked = cat([cat([er, ei], 1), cat([dr * c + di * s, di * c - dr * s], 1)], 0)
    z = dot3(split(stacked), b)
    return cat([z[:n, :h], z[n:, :h]], 1), cat([z[:n, h:], z[n:, h:]], 1)


def inverse_transform(fr, fi, a, b, rows, lanes):
    h = fr.shape[0] // 2
    n = 2 * h
    stacked = cat([cat([fr[:, :h], fi[:, :h]], 1), cat([fr[:, h:], fi[:, h:]], 1)], 0)
    z = dot3(split(stacked), a)
    er, ei, odr, odi = z[:n, :h], z[:n, h:], z[n:, :h], z[n:, h:]
    c, s = lanes
    tr, ti = odr * c - odi * s, odi * c + odr * s
    yr = cat([er + tr, er - tr], 1)
    yi = cat([ei + ti, ei - ti], 1)
    stacked = cat([cat([yr[:h], yr[h:]], 1), cat([yi[:h], yi[h:]], 1)], 0)
    v = dot3(b, split(stacked))
    er, ei, odr, odi = v[:h, :n], v[h:, :n], v[:h, n:], v[h:, n:]
    c, s = rows
    tr, ti = odr * c - odi * s, odi * c + odr * s
    return cat([er + tr, er - tr], 0), cat([ei + ti, ei - ti], 0)


def row_picker(count, depth, start, valid):
    place = lax.broadcasted_iota(jnp.int32, (count, depth), 0) - lax.broadcasted_iota(
        jnp.int32, (count, depth), 1
    )
    return jnp.where(place == start, valid, 0.0).astype(BF16)


def col_picker(depth, count, start):
    place = lax.broadcasted_iota(jnp.int32, (depth, count), 1) - lax.broadcasted_iota(
        jnp.int32, (depth, count), 0
    )
    return jnp.where(place == start, 1.0, 0.0).astype(BF16)


def corner(known, k, tile_rows, tile_cols, margin):
    row, col = lax.axis_index("row"), lax.axis_index("col")
    line = row + k // 2 - 1
    inside = (line >= 0) & (line < lax.axis_size("row"))
    mark = known[k]
    return (
        mark[0:1, 0:1] - (row * tile_rows + margin),
        mark[1:2, 0:1] - (col * tile_cols + margin),
        jnp.where(inside, 1.0, 0.0),
    )


def update_kernel(
    center, known, column, probe, amp, a_ref, b_ref, rows_ref, lanes_ref, shuffle,
    grad, numer, illum, peak, far, power, window,
):
    modes, side = probe.shape[1], probe.shape[2]
    half = side // 2
    a = (a_ref[0], a_ref[1])
    b = (b_ref[0], b_ref[1])
    rows = (rows_ref[0], rows_ref[1])
    lanes = (lanes_ref[0:1, :], lanes_ref[1:2, :])

    def wave(m):
        pr, pi = probe[0, m].astype(F32), probe[1, m].astype(F32)
        wr, wi = window[0], window[1]
        return pr, pi, wr, wi, pr * wr - pi * wi, pr * wi + pi * wr

    start = center[0, 0] - lax.axis_index("row") * illum.shape[0]
    base = pl.multiple_of(start // 8 * 8, 8)
    shift = lax.rem(side + 8 - lax.rem(start, 8), side + 8)
    for i in range(2):
        window[i] = pltpu.roll(column[i, pl.ds(base, side + 8), :], shift, 0)[:side]
    power[...] = jnp.zeros_like(power)

    def ahead(m, carry):
        pr, pi, wr, wi, xr, xi = wave(m)
        fr, fi = forward_transform(xr, xi, a, b, rows, lanes)
        far[0, m] = fr
        far[1, m] = fi
        power[0] += fr * fr + fi * fi
        power[1] += pr * pr + pi * pi
        return carry

    lax.fori_loop(0, modes, ahead, 0)
    measured = 0.0
    rest = amp[...]
    for i in range(3):
        piece = rest.astype(BF16)
        rest = rest - piece.astype(F32)
        measured += dot(dot(shuffle[1], piece).astype(BF16), shuffle[0])
    power[0] = measured / (jnp.sqrt(power[0]) + 0.5)
    high, low = split(power[1])
    tile_rows, tile_cols = illum.shape
    spot = cat([high, low], 1)
    illum[...] = jnp.zeros_like(illum)

    def place_spot(k, carry):
        top, left, valid = corner(known, k, tile_rows, tile_cols, half)
        picked = dot(row_picker(tile_rows, side, top, valid), spot).astype(BF16)
        across = col_picker(side, tile_cols, left)
        placed = dot(cat([picked[:, :side], picked[:, side:]], 0), across)
        illum[...] += placed[:tile_rows] + placed[tile_rows:]
        return carry

    lax.fori_loop(0, known.shape[0], place_spot, 0)
    peak[...] = jnp.full(peak.shape, jnp.max(illum[...]), F32)
    numer[...] = jnp.zeros_like(numer)

    def back(m, carry):
        pr, pi, wr, wi, xr, xi = wave(m)
        factor = power[0]
        gr, gi = inverse_transform(far[0, m] * factor, far[1, m] * factor, a, b, rows, lanes)
        dr, di = gr - xr, gi - xi
        numer[0] += pr * dr + pi * di
        numer[1] += pr * di - pi * dr
        ur = wr * dr + wi * di
        ui = wr * di - wi * dr
        for t in range(2):
            grad[t, pl.ds(pl.multiple_of(m * half, half), half), :] = ur[t * half : (t + 1) * half]
            grad[t, pl.ds(pl.multiple_of((modes + m) * half, half), half), :] = ui[
                t * half : (t + 1) * half
            ]
        return carry

    lax.fori_loop(0, modes, back, 0)
    weight = window[0] * window[0] + window[1] * window[1]
    top = 2 * modes * half
    for t in range(2):
        grad[t, top : top + half, :] = weight[t * half : (t + 1) * half]
        if grad.shape[1] > top + half:
            grad[t, top + half :, :] = jnp.zeros((grad.shape[1] - top - half, side), F32)


def gather_kernel(
    ring, marks, obj, column, known,
    strip, packed, near_s, near_r, tile_s, tile_r, pack_s, pack_r, pass_s, pass_r,
):
    row, col = lax.axis_index("row"), lax.axis_index("col")
    tile_rows, tile_cols = obj.shape[1:]
    side = column.shape[2]
    half = side // 2
    has = (row > 0, row < ring - 1)
    beside = (row - 1, row + 1)
    barrier = pltpu.get_barrier_semaphore()

    def greet(r, c):
        pl.semaphore_signal(
            barrier, inc=1, device_id={"row": r, "col": c}, device_id_type=MESH
        )

    greet(row, 1 - col)
    for t in range(2):

        @pl.when(has[t])
        def _():
            greet(beside[t], col)

    pl.semaphore_wait(barrier, 1 + jnp.where(has[0], 1, 0) + jnp.where(has[1], 1, 0))

    def remote(src, dst, s, r, to_row, to_col):
        return pltpu.make_async_remote_copy(
            src_ref=src, dst_ref=dst, send_sem=s, recv_sem=r,
            device_id={"row": to_row, "col": to_col}, device_id_type=MESH,
        )

    def own_lanes(c):
        return pl.ds(pl.multiple_of(half + c * tile_cols, 128), tile_cols)

    near = [
        remote(marks, known.at[2 * (1 - t), col], near_s.at[t], near_r.at[1 - t], beside[t], col)
        for t in range(2)
    ]
    mate_mark = remote(marks, known.at[1, col], near_s.at[2], near_r.at[2], row, 1 - col)
    tile = remote(obj, strip.at[:, :, own_lanes(col)], tile_s, tile_r, row, 1 - col)
    for t in range(2):

        @pl.when(has[t])
        def _():
            near[t].start()

    tile.start()
    mate_mark.start()
    strip[:, :, :half] = jnp.zeros((2, tile_rows, half), F32)
    strip[:, :, half + 2 * tile_cols :] = jnp.zeros((2, tile_rows, half), F32)
    strip[:, :, own_lanes(col)] = obj[...]
    tile.wait()

    def cut(mark):
        width = strip.shape[2]
        place = lax.broadcasted_iota(jnp.int32, (width, side), 0) - lax.broadcasted_iota(
            jnp.int32, (width, side), 1
        )
        pick = jnp.where(place == mark[1:2, 0:1], 1.0, 0.0).astype(BF16)
        rest, found = strip[...].reshape(2 * tile_rows, width), 0.0
        for _ in range(3):
            piece = rest.astype(BF16)
            rest = rest - piece.astype(F32)
            found += dot(piece, pick)
        return found.reshape(2, tile_rows, side)

    def pack(t):
        return remote(
            packed.at[t], column.at[:, pl.ds(2 * (1 - t) * tile_rows, tile_rows), :],
            pack_s.at[t], pack_r.at[1 - t], beside[t], col,
        )

    def arrived_pack(t):
        return remote(
            packed.at[1 - t], column.at[:, pl.ds(2 * t * tile_rows, tile_rows), :],
            pack_s.at[1 - t], pack_r.at[t], beside[t], col,
        )

    def share(t):
        here = known.at[2 * t, col]
        return remote(here, here, pass_s.at[t], pass_r.at[t], row, 1 - col)

    for t in range(2):

        @pl.when(has[t])
        def _():
            remote(
                marks, known.at[2 * t, col], near_s.at[1 - t], near_r.at[t], beside[t], col
            ).wait_recv()
            share(t).start()
            packed[t] = cut(known[2 * t, col])
            pack(t).start()

    known[1, col] = marks[...]
    column[:, tile_rows : 2 * tile_rows, :] = cut(marks[...])
    for t in range(2):

        @pl.when(jnp.logical_not(has[t]))
        def _():
            column[:, 2 * t * tile_rows : (2 * t + 1) * tile_rows, :] = jnp.zeros(
                (2, tile_rows, side), F32
            )

    mate_mark.wait()
    for t in range(2):

        @pl.when(has[t])
        def _():
            share(t).wait()

    for t in range(2):

        @pl.when(has[t])
        def _():
            pack(t).wait_send()
            remote(
                marks, known.at[2 * (1 - t), col], near_s.at[t], near_r.at[1 - t], beside[t], col
            ).wait_send()
            arrived_pack(t).wait_recv()


def ring_split(lines, ring):
    chunk = -(-lines // (16 * ring)) * 8
    pieces = min(2, chunk // 8)
    offsets, at = [], 0
    for i in range(pieces):
        size = (chunk // 8 // pieces + (1 if i < chunk // 8 % pieces else 0)) * 8
        offsets.append((at, size))
        at += size
    return chunk, offsets


def exchange_kernel(
    ring, chunk, pieces, grad, numer, peak, total, rims, mate, top,
    own, inbox, other, seen, highs, core_s, core_r, rs_s, rs_r, ag_s, ag_r, dd_s, dd_r,
    mine_s, mine_r, rim_s, rim_r, fwd_s, fwd_r, pk_s, pk_r,
):
    row, col = lax.axis_index("row"), lax.axis_index("col")
    side = grad.shape[2]
    half = side // 2
    mine = col
    odd = lax.rem(row, 2)
    at = jnp.where(odd == 1, ring - 1 - row // 2, row // 2)

    def row_at(p):
        p = lax.rem(p + ring, ring)
        return jnp.where(p < ring // 2, 2 * p, 2 * (ring - 1 - p) + 1)

    targets = (row_at(at + 1), row_at(at - 1))
    place = (at, lax.rem(ring - at, ring))
    has_up, has_down = row > 0, row < ring - 1

    barrier = pltpu.get_barrier_semaphore()

    def greet(r, c):
        pl.semaphore_signal(
            barrier, inc=1, device_id={"row": r, "col": c}, device_id_type=MESH
        )

    greet(row, 1 - col)
    greet(targets[0], col)
    greet(targets[1], col)

    @pl.when(has_up)
    def _():
        greet(row - 1, col)

    @pl.when(has_down)
    def _():
        greet(row + 1, col)

    pl.semaphore_wait(barrier, 3 + jnp.where(has_up, 1, 0) + jnp.where(has_down, 1, 0))

    def remote(src, dst, s, r, to_row, to_col):
        return pltpu.make_async_remote_copy(
            src_ref=src, dst_ref=dst, send_sem=s, recv_sem=r,
            device_id={"row": to_row, "col": to_col}, device_id_type=MESH,
        )

    first = remote(grad.at[1 - mine], other, core_s.at[0], core_r.at[0], row, 1 - col)
    first.start()
    peak_first = remote(peak, top, core_s.at[2], core_r.at[2], row, 1 - col)
    peak_first.start()
    numer_copy = remote(numer, mate, core_s.at[1], core_r.at[1], row, 1 - col)
    numer_copy.start()
    up = remote(
        numer.at[:, pl.ds(0, half), :], rims.at[mine, 1], rim_s.at[0], rim_r.at[1],
        row - 1, col,
    )
    down = remote(
        numer.at[:, pl.ds(half, half), :], rims.at[mine, 0], rim_s.at[1], rim_r.at[0],
        row + 1, col,
    )

    @pl.when(has_up)
    def _():
        up.start()

    @pl.when(has_down)
    def _():
        down.start()

    far = ring // 2

    def reach(b, d):
        return far if b == d else far - 1

    def spot(q, b, d, u):
        k = lax.rem(q + 2 * ring, ring)
        if d == 1:
            k = lax.rem(ring - k, ring)
        start = (k * 2 + b) * chunk + pieces[u][0]
        return pl.ds(pl.multiple_of(start, 8), pieces[u][1])

    def box(b, d, u):
        return pl.ds((2 * b + d) * chunk + pieces[u][0], pieces[u][1])

    flows = [(b, d, u) for u in range(len(pieces)) for b in range(2) for d in range(2)]

    def rs_copy(src, s, b, d, u):
        return remote(
            src, inbox.at[s, box(b, d, u), :], rs_s.at[s, b, d, u], rs_r.at[s, b, d, u],
            targets[d], col,
        )

    def rs_wait(s, b, d, u):
        return rs_copy(inbox.at[s, box(b, d, u), :], s, b, d, u)

    def ag_copy(s, b, d, u):
        here = total.at[mine, spot(place[d] - s, b, d, u), :]
        return remote(
            here, here, ag_s.at[s, b, d, u], ag_r.at[s, b, d, u], targets[d], col
        )

    def dd_copy(s, b, d, u):
        here = total.at[mine, spot(place[d] - 1 - s, b, d, u), :]
        return remote(here, here, dd_s.at[s, b, d, u], dd_r.at[s, b, d, u], row, 1 - col)

    def mine_copy(b, u):
        here = total.at[mine, spot(at, b, 0, u), :]
        return remote(here, here, mine_s.at[b, u], mine_r.at[b, u], row, 1 - col)

    def pk_copy(s, d):
        return remote(
            highs.at[s], seen.at[s, d], pk_s.at[s, d], pk_r.at[s, d], targets[d], col
        )

    peak_first.wait()
    highs[0] = jnp.maximum(peak[...], top[...])
    for d in range(2):
        pk_copy(0, d).start()
    first.wait()
    own[...] = grad[mine] + other[...]
    for b, d, u in flows:
        rs_copy(own.at[spot(place[d] + reach(b, d), b, d, u), :], 0, b, d, u).start()

    def pass_on(s, b, d, u):
        inbox[s, box(b, d, u), :] += own[spot(place[d] + reach(b, d) - s - 1, b, d, u), :]
        rs_copy(inbox.at[s, box(b, d, u), :], s + 1, b, d, u).start()

    def pass_peak(s):
        for d in range(2):
            pk_copy(s, d).wait_recv()
        highs[s + 1] = jnp.maximum(highs[s], jnp.maximum(seen[s, 0], seen[s, 1]))

    def scatter_step(s, carry):
        pass_peak(s)
        for d in range(2):
            pk_copy(s + 1, d).start()
        for b, d, u in flows:
            rs_wait(s, b, d, u).wait_recv()
            pass_on(s, b, d, u)
        return carry

    lax.fori_loop(0, far - 2, scatter_step, 0)
    pass_peak(far - 2)
    for d in range(2):
        pk_copy(far - 1, d).start()
    for b, d, u in flows:
        rs_wait(far - 2, b, d, u).wait_recv()
        if b == d:
            pass_on(far - 2, b, d, u)
    for u in range(len(pieces)):
        for b in range(2):
            rs_wait(far - 1, b, b, u).wait_recv()
            here = spot(at, b, 0, u)
            total[mine, here, :] = (
                own[here, :] + inbox[far - 1, box(b, b, u), :] + inbox[far - 2, box(b, 1 - b, u), :]
            )
            for d in range(2):
                ag_copy(0, b, d, u).start()
            mine_copy(b, u).start()
    pass_peak(far - 1)

    fwd = [
        remote(rims.at[mine, t], rims.at[mine, t], fwd_s.at[t], fwd_r.at[t], row, 1 - col)
        for t in range(2)
    ]

    @pl.when(has_down)
    def _():
        remote(
            numer.at[:, pl.ds(0, half), :], rims.at[mine, 1], rim_s.at[0], rim_r.at[1],
            row + 1, col,
        ).wait_recv()
        fwd[1].start()

    @pl.when(has_up)
    def _():
        remote(
            numer.at[:, pl.ds(half, half), :], rims.at[mine, 0], rim_s.at[1], rim_r.at[0],
            row - 1, col,
        ).wait_recv()
        fwd[0].start()

    def gather_step(s, carry):
        for b, d, u in flows:
            ag_copy(s, b, d, u).wait_recv()
            ag_copy(s + 1, b, d, u).start()
            dd_copy(s, b, d, u).start()
        return carry

    lax.fori_loop(0, far - 2, gather_step, 0)
    for b, d, u in flows:
        ag_copy(far - 2, b, d, u).wait_recv()
        if b == d:
            ag_copy(far - 1, b, d, u).start()
        dd_copy(far - 2, b, d, u).start()
    for b, d, u in flows:
        if b == d:
            ag_copy(far - 1, b, d, u).wait_recv()
            dd_copy(far - 1, b, d, u).start()

    def settle(s, b, d, u):
        rs_wait(s, b, d, u).wait_send()
        ag_copy(s, b, d, u).wait_send()
        dd_copy(s, b, d, u).wait()

    def finish(s, carry):
        for b, d, u in flows:
            settle(s, b, d, u)
        for d in range(2):
            pk_copy(s, d).wait_send()
        return carry

    lax.fori_loop(0, far - 1, finish, 0)
    for b, d, u in flows:
        if b == d:
            settle(far - 1, b, d, u)
    for d in range(2):
        pk_copy(far - 1, d).wait_send()
    for u in range(len(pieces)):
        for b in range(2):
            mine_copy(b, u).wait()
    numer_copy.wait()

    @pl.when(has_up)
    def _():
        up.wait_send()
        fwd[0].wait()

    @pl.when(has_down)
    def _():
        down.wait_send()
        fwd[1].wait()

    top[...] = highs[far]


def object_kernel(known, obj, numer, mate, rims, illum, top, out, acc):
    tile_rows, tile_cols = illum.shape
    side = numer.shape[2]
    half = side // 2
    mine = lax.axis_index("col")
    acc[...] = jnp.zeros_like(acc)

    def put(block, offset, k):
        top, left, valid = corner(known, k, tile_rows, tile_cols, half)
        block = jnp.where(valid > 0.0, block, 0.0)
        rh, rl = split(block[0])
        ih, il = split(block[1])
        stacked = cat([rh, ih, rl, il], 1)
        pick = row_picker(tile_rows, block.shape[1], top + offset, valid)
        picked = dot(pick, stacked).astype(BF16)
        tall = cat([picked[:, i * side : (i + 1) * side] for i in range(4)], 0)
        acc[...] += dot(tall, col_picker(side, tile_cols, left))

    for c in range(2):
        put(jnp.where(mine == c, numer[...], mate[...]), 0, 2 + c)
        put(rims[c, 0], half, c)
        put(rims[c, 1], 0, 4 + c)
    scale = 1.0 / (illum[...] + 0.1 * jnp.max(top[...]))
    for t in range(2):
        high = acc[t * tile_rows : (t + 1) * tile_rows]
        low = acc[(2 + t) * tile_rows : (3 + t) * tile_rows]
        out[t] = obj[t] + (high + low) * scale


def probe_kernel(probe, total, out):
    modes, side = probe.shape[1], probe.shape[2]
    half = side // 2
    top = 2 * modes * half
    biggest = jnp.max(
        jnp.maximum(total[0, top : top + half, :], total[1, top : top + half, :])
    )
    for t in range(2):
        scale = 1.0 / (total[t, top : top + half, :] + 0.1 * biggest)
        for i in range(2):
            for m in range(modes):
                line = (i * modes + m) * half
                out[i, m, t * half : (t + 1) * half, :] = (
                    probe[i, m, t * half : (t + 1) * half, :].astype(F32)
                    + total[t, line : line + half, :] * scale
                )


def struct(shape, kind=F32):
    return jax.ShapeDtypeStruct(shape, kind)


def local(obj_field, probe_modes, centers, amplitudes):
    tile_rows, tile_cols = obj_field.shape[1:]
    modes, side = probe_modes.shape[1:3]
    margin = side // 2
    ring, cores = lax.axis_size("row"), lax.axis_size("col")
    dma = pltpu.SemaphoreType.DMA
    lines_at = lax.broadcasted_iota(jnp.int32, (8, 128), 0)
    marks = jnp.where(lines_at == 0, centers[0, 0], centers[0, 1])
    column, known = pl.pallas_call(
        functools.partial(gather_kernel, ring),
        out_shape=(struct((2, 3 * tile_rows, side)), struct((3, cores, 8, 128), jnp.int32)),
        in_specs=[VMEM, VMEM],
        out_specs=(VMEM, VMEM),
        scratch_shapes=[
            pltpu.VMEM((2, tile_rows, cores * tile_cols + side), F32),
            pltpu.VMEM((2, 2, tile_rows, side), F32),
            dma((3,)), dma((3,)), dma, dma, dma((2,)), dma((2,)), dma((2,)), dma((2,)),
        ],
        compiler_params=pltpu.CompilerParams(
            vmem_limit_bytes=LIMIT, collective_id=2, has_side_effects=True
        ),
        name="gather",
    )(marks, obj_field)
    known = known.reshape(3 * cores, 8, 128)

    lines = (2 * modes + 1) * margin
    chunk, pieces = ring_split(lines, ring)
    depth = 2 * ring * chunk
    count = len(pieces)
    params = pltpu.CompilerParams(vmem_limit_bytes=LIMIT)
    grad, numer, illum, peak = pl.pallas_call(
        update_kernel,
        out_shape=(
            struct((2, depth, side)),
            struct((2, side, side)),
            struct((tile_rows, tile_cols)),
            struct((8, 128)),
        ),
        in_specs=[SMEM] + [VMEM] * 9,
        out_specs=(VMEM,) * 4,
        scratch_shapes=[
            pltpu.VMEM((2, modes, side, side), F32),
            pltpu.VMEM((2, side, side), F32),
            pltpu.VMEM((2, side, side), F32),
        ],
        compiler_params=params,
        name="update",
    )(centers, known, column, probe_modes, amplitudes[0], *tables(side))

    total, rims, mate, top = pl.pallas_call(
        functools.partial(exchange_kernel, ring, chunk, pieces),
        out_shape=(
            struct((2, depth, side)),
            struct((2, 2, 2, margin, side)),
            struct((2, side, side)),
            struct((8, 128)),
        ),
        in_specs=[VMEM] * 3,
        out_specs=(VMEM,) * 4,
        scratch_shapes=[
            pltpu.VMEM((depth, side), F32),
            pltpu.VMEM((ring // 2, 4 * chunk, side), F32),
            pltpu.VMEM((depth, side), F32),
            pltpu.VMEM((ring // 2, 2, 8, 128), F32),
            pltpu.VMEM((ring // 2 + 1, 8, 128), F32),
            dma((3,)), dma((3,)),
            *[dma((ring // 2, 2, 2, count))] * 6,
            dma((2, count)), dma((2, count)),
            dma((2,)), dma((2,)), dma((2,)), dma((2,)),
            dma((ring // 2, 2)), dma((ring // 2, 2)),
        ],
        compiler_params=pltpu.CompilerParams(
            vmem_limit_bytes=LIMIT, collective_id=1, has_side_effects=True
        ),
        name="exchange",
    )(grad, numer, peak)

    new_object = pl.pallas_call(
        object_kernel,
        out_shape=struct(obj_field.shape),
        in_specs=[VMEM] * 7,
        out_specs=VMEM,
        scratch_shapes=[pltpu.VMEM((4 * tile_rows, tile_cols), F32)],
        compiler_params=params,
        name="object",
    )(known, obj_field, numer, mate, rims, illum, top)
    new_probe = pl.pallas_call(
        probe_kernel,
        out_shape=struct(probe_modes.shape),
        in_specs=[VMEM] * 2,
        out_specs=VMEM,
        compiler_params=params,
        name="probe",
    )(probe_modes, total)
    return (new_object, new_probe)


def solution(mesh):
    in_specs = (
        P(None, ("angle", "row"), "col"),
        P(),
        P(("angle", "row", "col"), None),
        P(("angle", "row", "col"), None, None),
    )
    out_specs = (P(None, ("angle", "row"), "col"), P(None, "angle", None, None))
    return jax.shard_map(local, mesh=mesh, in_specs=in_specs, out_specs=out_specs, check_vma=False)
```

```python
import functools
import math

import jax
import jax.numpy as jnp
import numpy as np
from jax import lax
from jax.experimental import pallas as pl
from jax.experimental.pallas import tpu as pltpu
from jax.sharding import PartitionSpec as P

MESH = pl.DeviceIdType.MESH
F32 = jnp.float32
BF16 = jnp.bfloat16
VMEM = pl.BlockSpec(memory_space=pltpu.VMEM)
SMEM = pl.BlockSpec(memory_space=pltpu.SMEM)
LIMIT = 26 * 1024 * 1024


def split(x):
    high = x.astype(BF16)
    return high, (x - high.astype(F32)).astype(BF16)


def dot(a, b):
    return jnp.dot(a, b, preferred_element_type=F32)


def dot3(a, b):
    return dot(a[0], b[1]) + dot(a[1], b[0]) + dot(a[0], b[0])


def tables(side):
    half = side // 2
    k = np.arange(half)
    phase = (k[:, None] * k[None, :] % half) * (2.0 * math.pi / half)
    scale = 1.0 / math.sqrt(side)
    cosine, sine = np.cos(phase) * scale, np.sin(phase) * scale
    matrix = np.block([[cosine, sine], [-sine, cosine]]).astype(np.float32)
    turn = k * (2.0 * math.pi / side)
    lanes = np.stack([np.cos(turn), np.sin(turn)]).astype(np.float32)
    rows = np.ascontiguousarray(np.broadcast_to(lanes[:, :, None], (2, half, side)))
    order = np.concatenate([np.arange(0, side, 2), np.arange(1, side, 2)])
    shuffle = (np.arange(side)[:, None] == order[None, :]).astype(np.float32)
    high = matrix.astype(BF16)
    low = (matrix - high.astype(np.float32)).astype(BF16)
    return (
        jnp.asarray(np.stack([high, low])),
        jnp.asarray(np.stack([high.T, low.T])),
        jnp.asarray(rows),
        jnp.asarray(lanes),
        jnp.asarray(np.stack([shuffle, shuffle.T])).astype(BF16),
    )


def cat(parts, axis):
    return jnp.concatenate(parts, axis=axis)


def forward_transform(re, im, a, b, rows, lanes):
    h = re.shape[0] // 2
    n = 2 * h
    er, ei = re[:h] + re[h:], im[:h] + im[h:]
    dr, di = re[:h] - re[h:], im[:h] - im[h:]
    c, s = rows
    stacked = cat([cat([er, dr * c + di * s], 1), cat([ei, di * c - dr * s], 1)], 0)
    y = dot3(a, split(stacked))
    yr = cat([y[:h, :n], y[:h, n:]], 0)
    yi = cat([y[h:, :n], y[h:, n:]], 0)
    er, ei = yr[:, :h] + yr[:, h:], yi[:, :h] + yi[:, h:]
    dr, di = yr[:, :h] - yr[:, h:], yi[:, :h] - yi[:, h:]
    c, s = lanes
    stacked = cat([cat([er, ei], 1), cat([dr * c + di * s, di * c - dr * s], 1)], 0)
    z = dot3(split(stacked), b)
    return cat([z[:n, :h], z[n:, :h]], 1), cat([z[:n, h:], z[n:, h:]], 1)


def inverse_transform(fr, fi, a, b, rows, lanes):
    h = fr.shape[0] // 2
    n = 2 * h
    stacked = cat([cat([fr[:, :h], fi[:, :h]], 1), cat([fr[:, h:], fi[:, h:]], 1)], 0)
    z = dot3(split(stacked), a)
    er, ei, odr, odi = z[:n, :h], z[:n, h:], z[n:, :h], z[n:, h:]
    c, s = lanes
    tr, ti = odr * c - odi * s, odi * c + odr * s
    yr = cat([er + tr, er - tr], 1)
    yi = cat([ei + ti, ei - ti], 1)
    stacked = cat([cat([yr[:h], yr[h:]], 1), cat([yi[:h], yi[h:]], 1)], 0)
    v = dot3(b, split(stacked))
    er, ei, odr, odi = v[:h, :n], v[h:, :n], v[:h, n:], v[h:, n:]
    c, s = rows
    tr, ti = odr * c - odi * s, odi * c + odr * s
    return cat([er + tr, er - tr], 0), cat([ei + ti, ei - ti], 0)


def row_picker(count, depth, start, valid):
    place = lax.broadcasted_iota(jnp.int32, (count, depth), 0) - lax.broadcasted_iota(
        jnp.int32, (count, depth), 1
    )
    return jnp.where(place == start, valid, 0.0).astype(BF16)


def col_picker(depth, count, start):
    place = lax.broadcasted_iota(jnp.int32, (depth, count), 1) - lax.broadcasted_iota(
        jnp.int32, (depth, count), 0
    )
    return jnp.where(place == start, 1.0, 0.0).astype(BF16)


def corner(mark, k, tile_rows, tile_cols, margin):
    row, col = lax.axis_index("row"), lax.axis_index("col")
    line = row + k // 2 - 1
    inside = (line >= 0) & (line < lax.axis_size("row"))
    return (
        mark[0:1, 0:1] - (row * tile_rows + margin),
        mark[1:2, 0:1] - (col * tile_cols + margin),
        jnp.where(inside, 1.0, 0.0),
    )


def update_kernel(
    center, column, probe, amp, a_ref, b_ref, rows_ref, lanes_ref,
    grad, numer, far, power, window,
):
    modes, side = probe.shape[1], probe.shape[2]
    half = side // 2
    a = (a_ref[0], a_ref[1])
    b = (b_ref[0], b_ref[1])
    rows = (rows_ref[0], rows_ref[1])
    lanes = (lanes_ref[0:1, :], lanes_ref[1:2, :])

    def wave(m):
        pr, pi = probe[0, m].astype(F32), probe[1, m].astype(F32)
        wr, wi = window[0], window[1]
        return pr, pi, wr, wi, pr * wr - pi * wi, pr * wi + pi * wr

    start = center[0, 0] - lax.axis_index("row") * (column.shape[1] // 3)
    base = pl.multiple_of(start // 8 * 8, 8)
    shift = lax.rem(side + 8 - lax.rem(start, 8), side + 8)
    for i in range(2):
        window[i] = pltpu.roll(column[i, pl.ds(base, side + 8), :], shift, 0)[:side]
    power[...] = jnp.zeros_like(power)

    def ahead(m, carry):
        pr, pi, wr, wi, xr, xi = wave(m)
        fr, fi = forward_transform(xr, xi, a, b, rows, lanes)
        far[0, m] = fr
        far[1, m] = fi
        power[...] += fr * fr + fi * fi
        return carry

    lax.fori_loop(0, modes, ahead, 0)
    power[...] = amp[...] / (jnp.sqrt(power[...]) + 0.5)
    numer[...] = jnp.zeros_like(numer)

    def back(m, carry):
        pr, pi, wr, wi, xr, xi = wave(m)
        factor = power[...]
        gr, gi = inverse_transform(far[0, m] * factor, far[1, m] * factor, a, b, rows, lanes)
        dr, di = gr - xr, gi - xi
        numer[0] += pr * dr + pi * di
        numer[1] += pr * di - pi * dr
        ur = wr * dr + wi * di
        ui = wr * di - wi * dr
        for t in range(2):
            grad[t, pl.ds(pl.multiple_of(m * half, half), half), :] = ur[t * half : (t + 1) * half]
            grad[t, pl.ds(pl.multiple_of((modes + m) * half, half), half), :] = ui[
                t * half : (t + 1) * half
            ]
        return carry

    lax.fori_loop(0, modes, back, 0)
    weight = window[0] * window[0] + window[1] * window[1]
    top = 2 * modes * half
    for t in range(2):
        grad[t, top : top + half, :] = weight[t * half : (t + 1) * half]
        if grad.shape[1] > top + half:
            grad[t, top + half :, :] = jnp.zeros((grad.shape[1] - top - half, side), F32)


def gather_kernel(
    ring, marks, obj, probe_hbm, amp_hbm, shuffle_hbm, column, known, measured, illum, peak,
    strip, packed, near_s, near_r, tile_s, tile_r, pack_s, pack_r, pass_s, pass_r,
    probe, amp, shuffle, load_s,
):
    loads = [
        pltpu.make_async_copy(src, dst, load_s.at[i])
        for i, (src, dst) in enumerate(
            ((probe_hbm, probe), (amp_hbm, amp), (shuffle_hbm, shuffle))
        )
    ]
    for load in loads:
        load.start()
    row, col = lax.axis_index("row"), lax.axis_index("col")
    tile_rows, tile_cols = obj.shape[1:]
    side = column.shape[2]
    half = side // 2
    has = (row > 0, row < ring - 1)
    beside = (row - 1, row + 1)
    barrier = pltpu.get_barrier_semaphore()

    def greet(r, c):
        pl.semaphore_signal(
            barrier, inc=1, device_id={"row": r, "col": c}, device_id_type=MESH
        )

    greet(row, 1 - col)
    for t in range(2):

        @pl.when(has[t])
        def _():
            greet(beside[t], col)

    pl.semaphore_wait(barrier, 1 + jnp.where(has[0], 1, 0) + jnp.where(has[1], 1, 0))

    def remote(src, dst, s, r, to_row, to_col):
        return pltpu.make_async_remote_copy(
            src_ref=src, dst_ref=dst, send_sem=s, recv_sem=r,
            device_id={"row": to_row, "col": to_col}, device_id_type=MESH,
        )

    def own_lanes(c):
        return pl.ds(pl.multiple_of(half + c * tile_cols, 128), tile_cols)

    near = [
        remote(marks, known.at[2 * (1 - t), col], near_s.at[t], near_r.at[1 - t], beside[t], col)
        for t in range(2)
    ]
    mate_mark = remote(marks, known.at[1, col], near_s.at[2], near_r.at[2], row, 1 - col)
    tile = remote(obj, strip.at[:, :, own_lanes(col)], tile_s, tile_r, row, 1 - col)
    for t in range(2):

        @pl.when(has[t])
        def _():
            near[t].start()

    tile.start()
    mate_mark.start()
    strip[:, :, :half] = jnp.zeros((2, tile_rows, half), F32)
    strip[:, :, half + 2 * tile_cols :] = jnp.zeros((2, tile_rows, half), F32)
    strip[:, :, own_lanes(col)] = obj[...]
    tile.wait()

    def cut(mark):
        width = strip.shape[2]
        place = lax.broadcasted_iota(jnp.int32, (width, side), 0) - lax.broadcasted_iota(
            jnp.int32, (width, side), 1
        )
        pick = jnp.where(place == mark[1:2, 0:1], 1.0, 0.0).astype(BF16)
        rest, found = strip[...].reshape(2 * tile_rows, width), 0.0
        for _ in range(3):
            piece = rest.astype(BF16)
            rest = rest - piece.astype(F32)
            found += dot(piece, pick)
        return found.reshape(2, tile_rows, side)

    def pack(t):
        return remote(
            packed.at[t], column.at[:, pl.ds(2 * (1 - t) * tile_rows, tile_rows), :],
            pack_s.at[t], pack_r.at[1 - t], beside[t], col,
        )

    def arrived_pack(t):
        return remote(
            packed.at[1 - t], column.at[:, pl.ds(2 * t * tile_rows, tile_rows), :],
            pack_s.at[1 - t], pack_r.at[t], beside[t], col,
        )

    def share(t):
        here = known.at[2 * t, col]
        return remote(here, here, pass_s.at[t], pass_r.at[t], row, 1 - col)

    for t in range(2):

        @pl.when(has[t])
        def _():
            remote(
                marks, known.at[2 * t, col], near_s.at[1 - t], near_r.at[t], beside[t], col
            ).wait_recv()
            share(t).start()
            packed[t] = cut(known[2 * t, col])
            pack(t).start()

    known[1, col] = marks[...]
    column[:, tile_rows : 2 * tile_rows, :] = cut(marks[...])
    for t in range(2):

        @pl.when(jnp.logical_not(has[t]))
        def _():
            column[:, 2 * t * tile_rows : (2 * t + 1) * tile_rows, :] = jnp.zeros(
                (2, tile_rows, side), F32
            )

    for load in loads:
        load.wait()
    found, rest = 0.0, amp[...]
    for i in range(3):
        piece = rest.astype(BF16)
        rest = rest - piece.astype(F32)
        found += dot(dot(shuffle[1], piece).astype(BF16), shuffle[0])
    measured[...] = found
    spot = 0.0
    for m in range(probe.shape[1]):
        pr, pi = probe[0, m].astype(F32), probe[1, m].astype(F32)
        spot += pr * pr + pi * pi
    spot = cat(split(spot), 1)
    mate_mark.wait()
    for t in range(2):

        @pl.when(has[t])
        def _():
            share(t).wait()

    total = 0.0
    for k in range(6):
        top, left, valid = corner(known[k // 2, k % 2], k, tile_rows, tile_cols, half)
        picked = dot(row_picker(tile_rows, side, top, valid), spot).astype(BF16)
        tall = cat([picked[:, :side], picked[:, side:]], 0)
        placed = dot(tall, col_picker(side, tile_cols, left))
        total += placed[:tile_rows] + placed[tile_rows:]
    illum[...] = total
    peak[...] = jnp.full(peak.shape, jnp.max(total), F32)

    for t in range(2):

        @pl.when(has[t])
        def _():
            pack(t).wait_send()
            remote(
                marks, known.at[2 * (1 - t), col], near_s.at[t], near_r.at[1 - t], beside[t], col
            ).wait_send()
            arrived_pack(t).wait_recv()


def ring_split(lines, ring):
    chunk = -(-lines // (16 * ring)) * 8
    pieces = min(2, chunk // 8)
    offsets, at = [], 0
    for i in range(pieces):
        size = (chunk // 8 // pieces + (1 if i < chunk // 8 % pieces else 0)) * 8
        offsets.append((at, size))
        at += size
    return chunk, offsets


def exchange_kernel(
    ring, chunk, pieces, known, grad, numer, peak, total, acc, top,
    rims, mate,
    own, inbox, other, seen, highs, core_s, core_r, rs_s, rs_r, ag_s, ag_r, dd_s, dd_r,
    mine_s, mine_r, rim_s, rim_r, fwd_s, fwd_r, pk_s, pk_r,
):
    row, col = lax.axis_index("row"), lax.axis_index("col")
    side = grad.shape[2]
    half = side // 2
    mine = col
    odd = lax.rem(row, 2)
    at = jnp.where(odd == 1, ring - 1 - row // 2, row // 2)

    def row_at(p):
        p = lax.rem(p + ring, ring)
        return jnp.where(p < ring // 2, 2 * p, 2 * (ring - 1 - p) + 1)

    targets = (row_at(at + 1), row_at(at - 1))
    place = (at, lax.rem(ring - at, ring))
    has_up, has_down = row > 0, row < ring - 1

    barrier = pltpu.get_barrier_semaphore()

    def greet(r, c):
        pl.semaphore_signal(
            barrier, inc=1, device_id={"row": r, "col": c}, device_id_type=MESH
        )

    greet(row, 1 - col)
    greet(targets[0], col)
    greet(targets[1], col)

    @pl.when(has_up)
    def _():
        greet(row - 1, col)

    @pl.when(has_down)
    def _():
        greet(row + 1, col)

    pl.semaphore_wait(barrier, 3 + jnp.where(has_up, 1, 0) + jnp.where(has_down, 1, 0))

    def remote(src, dst, s, r, to_row, to_col):
        return pltpu.make_async_remote_copy(
            src_ref=src, dst_ref=dst, send_sem=s, recv_sem=r,
            device_id={"row": to_row, "col": to_col}, device_id_type=MESH,
        )

    first = remote(grad.at[1 - mine], other, core_s.at[0], core_r.at[0], row, 1 - col)
    first.start()
    peak_first = remote(peak, top, core_s.at[2], core_r.at[2], row, 1 - col)
    peak_first.start()
    numer_copy = remote(numer, mate, core_s.at[1], core_r.at[1], row, 1 - col)
    numer_copy.start()
    up = remote(
        numer.at[:, pl.ds(0, half), :], rims.at[mine, 1], rim_s.at[0], rim_r.at[1],
        row - 1, col,
    )
    down = remote(
        numer.at[:, pl.ds(half, half), :], rims.at[mine, 0], rim_s.at[1], rim_r.at[0],
        row + 1, col,
    )

    @pl.when(has_up)
    def _():
        up.start()

    @pl.when(has_down)
    def _():
        down.start()

    far = ring // 2

    def reach(b, d):
        return far if b == d else far - 1

    def spot(q, b, d, u):
        k = lax.rem(q + 2 * ring, ring)
        if d == 1:
            k = lax.rem(ring - k, ring)
        start = (k * 2 + b) * chunk + pieces[u][0]
        return pl.ds(pl.multiple_of(start, 8), pieces[u][1])

    def box(b, d, u):
        return pl.ds((2 * b + d) * chunk + pieces[u][0], pieces[u][1])

    flows = [(b, d, u) for u in range(len(pieces)) for b in range(2) for d in range(2)]

    def rs_copy(src, s, b, d, u):
        return remote(
            src, inbox.at[s, box(b, d, u), :], rs_s.at[s, b, d, u], rs_r.at[s, b, d, u],
            targets[d], col,
        )

    def rs_wait(s, b, d, u):
        return rs_copy(inbox.at[s, box(b, d, u), :], s, b, d, u)

    def ag_copy(s, b, d, u):
        here = total.at[mine, spot(place[d] - s, b, d, u), :]
        return remote(
            here, here, ag_s.at[s, b, d, u], ag_r.at[s, b, d, u], targets[d], col
        )

    def dd_copy(s, b, d, u):
        here = total.at[mine, spot(place[d] - 1 - s, b, d, u), :]
        return remote(here, here, dd_s.at[s, b, d, u], dd_r.at[s, b, d, u], row, 1 - col)

    def mine_copy(b, u):
        here = total.at[mine, spot(at, b, 0, u), :]
        return remote(here, here, mine_s.at[b, u], mine_r.at[b, u], row, 1 - col)

    def pk_copy(s, d):
        return remote(
            highs.at[s], seen.at[s, d], pk_s.at[s, d], pk_r.at[s, d], targets[d], col
        )

    peak_first.wait()
    highs[0] = jnp.maximum(peak[...], top[...])
    for d in range(2):
        pk_copy(0, d).start()
    first.wait()
    own[...] = grad[mine] + other[...]
    for b, d, u in flows:
        rs_copy(own.at[spot(place[d] + reach(b, d), b, d, u), :], 0, b, d, u).start()

    def pass_on(s, b, d, u):
        inbox[s, box(b, d, u), :] += own[spot(place[d] + reach(b, d) - s - 1, b, d, u), :]
        rs_copy(inbox.at[s, box(b, d, u), :], s + 1, b, d, u).start()

    def pass_peak(s):
        for d in range(2):
            pk_copy(s, d).wait_recv()
        highs[s + 1] = jnp.maximum(highs[s], jnp.maximum(seen[s, 0], seen[s, 1]))

    def scatter_step(s, carry):
        pass_peak(s)
        for d in range(2):
            pk_copy(s + 1, d).start()
        for b, d, u in flows:
            rs_wait(s, b, d, u).wait_recv()
            pass_on(s, b, d, u)
        return carry

    lax.fori_loop(0, far - 2, scatter_step, 0)
    pass_peak(far - 2)
    for d in range(2):
        pk_copy(far - 1, d).start()
    for b, d, u in flows:
        rs_wait(far - 2, b, d, u).wait_recv()
        if b == d:
            pass_on(far - 2, b, d, u)
    for u in range(len(pieces)):
        for b in range(2):
            rs_wait(far - 1, b, b, u).wait_recv()
            here = spot(at, b, 0, u)
            total[mine, here, :] = (
                own[here, :] + inbox[far - 1, box(b, b, u), :] + inbox[far - 2, box(b, 1 - b, u), :]
            )
            for d in range(2):
                ag_copy(0, b, d, u).start()
            mine_copy(b, u).start()
    pass_peak(far - 1)

    fwd = [
        remote(rims.at[mine, t], rims.at[mine, t], fwd_s.at[t], fwd_r.at[t], row, 1 - col)
        for t in range(2)
    ]

    @pl.when(has_down)
    def _():
        remote(
            numer.at[:, pl.ds(0, half), :], rims.at[mine, 1], rim_s.at[0], rim_r.at[1],
            row + 1, col,
        ).wait_recv()
        fwd[1].start()

    @pl.when(has_up)
    def _():
        remote(
            numer.at[:, pl.ds(half, half), :], rims.at[mine, 0], rim_s.at[1], rim_r.at[0],
            row - 1, col,
        ).wait_recv()
        fwd[0].start()

    def gather_step(s, carry):
        for b, d, u in flows:
            ag_copy(s, b, d, u).wait_recv()
            ag_copy(s + 1, b, d, u).start()
            dd_copy(s, b, d, u).start()
        return carry

    lax.fori_loop(0, far - 2, gather_step, 0)
    for b, d, u in flows:
        ag_copy(far - 2, b, d, u).wait_recv()
        if b == d:
            ag_copy(far - 1, b, d, u).start()
        dd_copy(far - 2, b, d, u).start()
    tile_rows, tile_cols = acc.shape[0] // 4, acc.shape[1]

    def put(block, offset, k):
        top, left, valid = corner(known[k], k, tile_rows, tile_cols, half)
        block = jnp.where(valid > 0.0, block, 0.0)
        rh, rl = split(block[0])
        ih, il = split(block[1])
        stacked = cat([rh, ih, rl, il], 1)
        pick = row_picker(tile_rows, block.shape[1], top + offset, valid)
        picked = dot(pick, stacked).astype(BF16)
        tall = cat([picked[:, i * side : (i + 1) * side] for i in range(4)], 0)
        acc[...] += dot(tall, col_picker(side, tile_cols, left))

    numer_copy.wait()
    for t in range(2):

        @pl.when((has_up, has_down)[t])
        def _():
            fwd[t].wait()

    acc[...] = jnp.zeros_like(acc)
    for c in range(2):
        put(jnp.where(mine == c, numer[...], mate[...]), 0, 2 + c)
        put(rims[c, 0], half, c)
        put(rims[c, 1], 0, 4 + c)

    for b, d, u in flows:
        if b == d:
            ag_copy(far - 1, b, d, u).wait_recv()
            dd_copy(far - 1, b, d, u).start()

    def settle(s, b, d, u):
        rs_wait(s, b, d, u).wait_send()
        ag_copy(s, b, d, u).wait_send()
        dd_copy(s, b, d, u).wait()

    def finish(s, carry):
        for b, d, u in flows:
            settle(s, b, d, u)
        for d in range(2):
            pk_copy(s, d).wait_send()
        return carry

    lax.fori_loop(0, far - 1, finish, 0)
    for b, d, u in flows:
        if b == d:
            settle(far - 1, b, d, u)
    for d in range(2):
        pk_copy(far - 1, d).wait_send()
    for u in range(len(pieces)):
        for b in range(2):
            mine_copy(b, u).wait()

    @pl.when(has_up)
    def _():
        up.wait_send()

    @pl.when(has_down)
    def _():
        down.wait_send()

    top[...] = highs[far]


def object_kernel(obj, acc, illum, top, out):
    tile_rows = illum.shape[0]
    scale = 1.0 / (illum[...] + 0.1 * jnp.max(top[...]))
    for t in range(2):
        high = acc[t * tile_rows : (t + 1) * tile_rows]
        low = acc[(2 + t) * tile_rows : (3 + t) * tile_rows]
        out[t] = obj[t] + (high + low) * scale


def probe_kernel(probe, total, out):
    modes, side = probe.shape[1], probe.shape[2]
    half = side // 2
    top = 2 * modes * half
    biggest = jnp.max(
        jnp.maximum(total[0, top : top + half, :], total[1, top : top + half, :])
    )
    for t in range(2):
        scale = 1.0 / (total[t, top : top + half, :] + 0.1 * biggest)
        for i in range(2):
            for m in range(modes):
                line = (i * modes + m) * half
                out[i, m, t * half : (t + 1) * half, :] = (
                    probe[i, m, t * half : (t + 1) * half, :].astype(F32)
                    + total[t, line : line + half, :] * scale
                )


def struct(shape, kind=F32):
    return jax.ShapeDtypeStruct(shape, kind)


def local(obj_field, probe_modes, centers, amplitudes):
    tile_rows, tile_cols = obj_field.shape[1:]
    modes, side = probe_modes.shape[1:3]
    margin = side // 2
    ring, cores = lax.axis_size("row"), lax.axis_size("col")
    dma = pltpu.SemaphoreType.DMA
    lines_at = lax.broadcasted_iota(jnp.int32, (8, 128), 0)
    marks = jnp.where(lines_at == 0, centers[0, 0], centers[0, 1])
    *consts, shuffle = tables(side)
    column, known, measured, illum, peak = pl.pallas_call(
        functools.partial(gather_kernel, ring),
        out_shape=(
            struct((2, 3 * tile_rows, side)),
            struct((3, cores, 8, 128), jnp.int32),
            struct((side, side)),
            struct((tile_rows, tile_cols)),
            struct((8, 128)),
        ),
        in_specs=[VMEM] * 2 + [pl.BlockSpec(memory_space=pltpu.HBM)] * 3,
        out_specs=(VMEM,) * 5,
        scratch_shapes=[
            pltpu.VMEM((2, tile_rows, cores * tile_cols + side), F32),
            pltpu.VMEM((2, 2, tile_rows, side), F32),
            dma((3,)), dma((3,)), dma, dma, dma((2,)), dma((2,)), dma((2,)), dma((2,)),
            pltpu.VMEM(probe_modes.shape, BF16),
            pltpu.VMEM((side, side), F32),
            pltpu.VMEM((2, side, side), BF16),
            dma((3,)),
        ],
        compiler_params=pltpu.CompilerParams(
            vmem_limit_bytes=LIMIT, collective_id=2, has_side_effects=True
        ),
        cost_estimate=pl.CostEstimate(
            flops=4 * 10**9, bytes_accessed=40 * 10**6, transcendentals=0
        ),
        name="gather",
    )(marks, obj_field, probe_modes, amplitudes[0], shuffle)
    known = known.reshape(3 * cores, 8, 128)

    lines = (2 * modes + 1) * margin
    chunk, pieces = ring_split(lines, ring)
    depth = 2 * ring * chunk
    count = len(pieces)
    params = pltpu.CompilerParams(vmem_limit_bytes=LIMIT)
    grad, numer = pl.pallas_call(
        update_kernel,
        out_shape=(
            struct((2, depth, side)),
            struct((2, side, side)),
        ),
        in_specs=[SMEM] + [VMEM] * 7,
        out_specs=(VMEM,) * 2,
        scratch_shapes=[
            pltpu.VMEM((2, modes, side, side), F32),
            pltpu.VMEM((side, side), F32),
            pltpu.VMEM((2, side, side), F32),
        ],
        compiler_params=params,
        name="update",
    )(centers, column, probe_modes, measured, *consts)

    total, acc, top = pl.pallas_call(
        functools.partial(exchange_kernel, ring, chunk, pieces),
        out_shape=(
            struct((2, depth, side)),
            struct((4 * tile_rows, tile_cols)),
            struct((8, 128)),
        ),
        in_specs=[VMEM] * 4,
        out_specs=(VMEM,) * 3,
        scratch_shapes=[
            pltpu.VMEM((2, 2, 2, margin, side), F32),
            pltpu.VMEM((2, side, side), F32),
            pltpu.VMEM((depth, side), F32),
            pltpu.VMEM((ring // 2, 4 * chunk, side), F32),
            pltpu.VMEM((depth, side), F32),
            pltpu.VMEM((ring // 2, 2, 8, 128), F32),
            pltpu.VMEM((ring // 2 + 1, 8, 128), F32),
            dma((3,)), dma((3,)),
            *[dma((ring // 2, 2, 2, count))] * 6,
            dma((2, count)), dma((2, count)),
            dma((2,)), dma((2,)), dma((2,)), dma((2,)),
            dma((ring // 2, 2)), dma((ring // 2, 2)),
        ],
        compiler_params=pltpu.CompilerParams(
            vmem_limit_bytes=LIMIT, collective_id=1, has_side_effects=True
        ),
        name="exchange",
    )(known, grad, numer, peak)

    new_object = pl.pallas_call(
        object_kernel,
        out_shape=struct(obj_field.shape),
        in_specs=[VMEM] * 4,
        out_specs=VMEM,
        compiler_params=params,
        name="object",
    )(obj_field, acc, illum, top)
    new_probe = pl.pallas_call(
        probe_kernel,
        out_shape=struct(probe_modes.shape),
        in_specs=[VMEM] * 2,
        out_specs=VMEM,
        compiler_params=params,
        name="probe",
    )(probe_modes, total)
    return (new_object, new_probe)


def solution(mesh):
    in_specs = (
        P(None, ("angle", "row"), "col"),
        P(),
        P(("angle", "row", "col"), None),
        P(("angle", "row", "col"), None, None),
    )
    out_specs = (P(None, ("angle", "row"), "col"), P(None, "angle", None, None))
    return jax.shard_map(local, mesh=mesh, in_specs=in_specs, out_specs=out_specs, check_vma=False)
```
